16 devices in a mesh: dp: 2 (over y, z), cp: 8 (over x, core).
Axes of the slice: x: 4, y: 2, z: 1, core: 2. Of those that a mesh axis runs over, the one named last changes fastest.
The devices are a block of a 4x4x8 slice.
Arguments:
- q_tok: bfloat16 [16384, 3, 128], P(('dp', 'cp')), parts along dimension 0
- k_tok: bfloat16 [16384, 128], P(('dp', 'cp')), parts along dimension 0
- v_tok: bfloat16 [16384, 128], P(('dp', 'cp')), parts along dimension 0
- fwd_out: bfloat16 [16384, 3, 128], P(('dp', 'cp')), parts along dimension 0
- d_out: bfloat16 [16384, 3, 128], P(('dp', 'cp')), parts along dimension 0
- lse_row: float32 [16384, 3], P(('dp', 'cp')), parts along dimension 0
Outputs:
- output 1: bfloat16 [16384, 3, 128], P(('dp', 'cp')), parts along dimension 0
- output 2: bfloat16 [16384, 128], P(('dp', 'cp')), parts along dimension 0
- output 3: bfloat16 [16384, 128], P(('dp', 'cp')), parts along dimension 0
There are 2 independent parts. The reference program is written for one: setup_inputs(seed, part) draws one part's arguments, and reference() takes and returns one part's arrays. A program takes and returns all parts, laid end to end along the dimension named above; each array names one.
All inputs are finite; a program needn't handle non-finite values.
Results may differ from the reference program's by a relative error of at most 0.001.
Values are sent between devices in bfloat16 or wider.
A program may use at most 768 MiB of HBM per device.

```python
import jax
import jax.numpy as jnp
from jax import lax

TOK_DEV = 1024
CP = 8
GQA = 3
HEAD = 128

SEQ = CP * TOK_DEV
Q_BLOCK = min(TOK_DEV, 128)
SOFTMAX_SCALE = HEAD ** -0.5
GRAD_GAIN = 0.25 * SEQ ** 0.5


def attention_forward(q_tok, k_tok, v_tok):
    k_full = k_tok.astype(jnp.float32)
    v_full = v_tok.astype(jnp.float32)
    columns = jnp.arange(SEQ)
    n_blocks = SEQ // Q_BLOCK

    def one_block(block_in):
        q_block, row_ids = block_in
        logits = jnp.einsum('rgd,cd->rgc', q_block.astype(jnp.float32), k_full) * SOFTMAX_SCALE
        allowed = columns[None, :] <= row_ids[:, None]
        logits = jnp.where(allowed[:, None, :], logits, -jnp.inf)
        lse_block = jax.nn.logsumexp(logits, axis=-1)
        prob_mat = jnp.exp(logits - lse_block[:, :, None])
        out_block = jnp.einsum('rgc,cd->rgd', prob_mat, v_full)
        return out_block.astype(jnp.bfloat16), lse_block

    out_blocks, lse_blocks = lax.map(one_block, (q_tok.reshape(n_blocks, Q_BLOCK, GQA, HEAD), columns.reshape(n_blocks, Q_BLOCK)))
    return out_blocks.reshape(SEQ, GQA, HEAD), lse_blocks.reshape(SEQ, GQA)


def setup_inputs(seed: int = 0, part: int = 0) -> dict:
    base_key = jax.random.fold_in(jax.random.key(seed), part)
    key_q, key_k, key_v, key_m, key_g = jax.random.split(base_key, 5)
    q_tok = jax.random.normal(key_q, (SEQ, GQA, HEAD), jnp.float32).astype(jnp.bfloat16)
    k_tok = jax.random.normal(key_k, (SEQ, HEAD), jnp.float32).astype(jnp.bfloat16)
    v_mean = jax.random.normal(key_m, (HEAD,), jnp.float32)
    v_tok = (v_mean[None, :] + jax.random.normal(key_v, (SEQ, HEAD), jnp.float32)).astype(jnp.bfloat16)
    d_out = (GRAD_GAIN * jax.random.normal(key_g, (SEQ, GQA, HEAD), jnp.float32)).astype(jnp.bfloat16)
    fwd_out, lse_row = attention_forward(q_tok, k_tok, v_tok)
    return {'q_tok': q_tok, 'k_tok': k_tok, 'v_tok': v_tok, 'fwd_out': fwd_out, 'd_out': d_out, 'lse_row': lse_row}


def reference(q_tok, k_tok, v_tok, fwd_out, d_out, lse_row):
    row_delta = jnp.sum(d_out.astype(jnp.float32) * fwd_out.astype(jnp.float32), axis=-1)
    k_full = k_tok.astype(jnp.float32)
    v_full = v_tok.astype(jnp.float32)
    columns = jnp.arange(SEQ)
    n_blocks = SEQ // Q_BLOCK

    def one_block(carry, block_in):
        dk_acc, dv_acc = carry
        q_block, do_block, lse_block, delta_block, row_ids = block_in
        q_wide = q_block.astype(jnp.float32)
        do_wide = do_block.astype(jnp.float32)
        logits = jnp.einsum('rgd,cd->rgc', q_wide, k_full) * SOFTMAX_SCALE
        allowed = columns[None, :] <= row_ids[:, None]
        prob_mat = jnp.exp(jnp.where(allowed[:, None, :], logits - lse_block[:, :, None], -jnp.inf))
        d_prob = jnp.einsum('rgd,cd->rgc', do_wide, v_full)
        d_score = prob_mat * (d_prob - delta_block[:, :, None])
        prob_low = prob_mat.astype(jnp.bfloat16).astype(jnp.float32)
        score_low = d_score.astype(jnp.bfloat16).astype(jnp.float32)
        dq_block = jnp.einsum('rgc,cd->rgd', score_low, k_full) * SOFTMAX_SCALE
        dk_acc = dk_acc + jnp.einsum('rgc,rgd->cd', score_low, q_wide)
        dv_acc = dv_acc + jnp.einsum('rgc,rgd->cd', prob_low, do_wide)
        return (dk_acc, dv_acc), dq_block.astype(jnp.bfloat16)

    acc_start = (jnp.zeros((SEQ, HEAD), jnp.float32), jnp.zeros((SEQ, HEAD), jnp.float32))
    block_inputs = (q_tok.reshape(n_blocks, Q_BLOCK, GQA, HEAD), d_out.reshape(n_blocks, Q_BLOCK, GQA, HEAD), lse_row.reshape(n_blocks, Q_BLOCK, GQA), row_delta.reshape(n_blocks, Q_BLOCK, GQA), columns.reshape(n_blocks, Q_BLOCK))
    (dk_acc, dv_acc), dq_blocks = lax.scan(one_block, acc_start, block_inputs)
    grad_q = dq_blocks.reshape(SEQ, GQA, HEAD)
    grad_k = (dk_acc * SOFTMAX_SCALE).astype(jnp.bfloat16)
    grad_v = dv_acc.astype(jnp.bfloat16)
    return (grad_q, grad_k, grad_v)
```

```python
import functools
import math

import jax
import jax.numpy as jnp
from jax import lax
from jax.experimental import pallas as pl
from jax.experimental.pallas import tpu as pltpu
from jax.sharding import PartitionSpec as P

NT = (((1,), (1,)), ((), ()))
NN = (((1,), (0,)), ((), ()))
LOG2E = math.log2(math.e)
A, B, R = 0, 1, 2


def dot(a, b, dims):
    return lax.dot_general(a, b, dims, preferred_element_type=jnp.float32)


def kernel(n_dev, q_hbm, do_hbm, ld_hbm, k_hbm, v_hbm, gq, gk, gv,
           q, do, qt, dot_t, ld, lseb, delb, kv, acc, dq, rbuf, rhalf, rdq,
           in_sem, pair_send, pair_recv, kv_send, kv_recv, g_send, g_recv, f_send, d_send, d_recv):
    heads, rows, dim = q.shape[1:]
    half = rows // 2
    scale = dim ** -0.5
    scale2 = scale * LOG2E
    own_slot = n_dev // 2
    n_chip = n_dev // 2

    me = lax.axis_index('cp')
    chip, core = me // 2, me % 2
    other = 1 - core
    partner = chip * 2 + other

    def at(chip_id):
        return {'cp': chip_id * 2 + core}

    loads = [
        pltpu.make_async_copy(k_hbm, kv.at[own_slot + core, 0], in_sem.at[0]),
        pltpu.make_async_copy(v_hbm, kv.at[own_slot + core, 1], in_sem.at[1]),
        pltpu.make_async_copy(q_hbm, q.at[core], in_sem.at[2]),
        pltpu.make_async_copy(do_hbm, do.at[core], in_sem.at[3]),
        pltpu.make_async_copy(ld_hbm, ld.at[core], in_sem.at[4]),
    ]
    for copy in loads:
        copy.start()

    barrier = pltpu.get_barrier_semaphore()
    for d in range(1, n_dev):
        pl.semaphore_signal(barrier, inc=1, device_id={'cp': lax.rem(me + d, n_dev)}, device_id_type=pl.DeviceIdType.MESH)
    acc[...] = jnp.zeros_like(acc)
    dq[...] = jnp.zeros_like(dq)
    pl.semaphore_wait(barrier, n_dev - 1)

    def remote(src, dst, send, recv, device):
        return pltpu.make_async_remote_copy(src_ref=src, dst_ref=dst, send_sem=send, recv_sem=recv,
                                            device_id=device, device_id_type=pl.DeviceIdType.MESH)

    def kv_copies(slot, src_slot, sem_row, device):
        return [remote(kv.at[src_slot, i], kv.at[slot, i], kv_send.at[sem_row, i], kv_recv.at[slot, i], device)
                for i in range(2)]

    def kv_send_own(sem_row, to_chip):
        for copy in kv_copies(chip, own_slot + core, sem_row, at(to_chip)):
            copy.start()

    def kv_wait_sent(sem_row):
        for copy in kv_copies(0, 0, sem_row, at(chip)):
            copy.wait_send()

    last = n_chip - 1
    late_next = jnp.logical_and(chip == last - 1, core == 0)
    late_wrap = jnp.logical_and(chip == 0, core == 1)
    loads[0].wait()
    loads[1].wait()

    @pl.when(jnp.logical_and(chip < last, jnp.logical_not(late_next)))
    def _():
        kv_send_own(0, chip + 1)

    @pl.when(jnp.logical_and(chip == 0, core == 0))
    def _():
        kv_send_own(1, last)

    pair = [
        remote(kv.at[own_slot + core, 0], kv.at[own_slot + core, 0], pair_send.at[0], pair_recv.at[0], {'cp': partner}),
        remote(kv.at[own_slot + core, 1], kv.at[own_slot + core, 1], pair_send.at[1], pair_recv.at[1], {'cp': partner}),
        remote(q.at[core], q.at[core], pair_send.at[2], pair_recv.at[2], {'cp': partner}),
        remote(do.at[core], do.at[core], pair_send.at[3], pair_recv.at[3], {'cp': partner}),
        remote(ld.at[core], ld.at[core], pair_send.at[4], pair_recv.at[4], {'cp': partner}),
    ]
    for i in (2, 3, 4):
        loads[i].wait()
        pair[i].start()
    pair[0].start()
    pair[1].start()

    def prep(b):
        qt[b] = q[b].reshape(heads * rows, dim).T
        dot_t[b] = do[b].reshape(heads * rows, dim).T
        for g in range(heads):
            lseb[b, g] = jnp.broadcast_to(ld[b, :, g:g + 1], (rows, dim))
            delb[b, g] = jnp.broadcast_to(ld[b, :, heads + g:heads + g + 1], (rows, dim))

    def tile(b, row_half, slot, h, masked):
        size = rows if row_half is None else half
        first = 0 if row_half is None else row_half * half
        start = pl.multiple_of(h * half, half)
        kk = kv[slot, 0, pl.ds(start, half), :]
        vv = kv[slot, 1, pl.ds(start, half), :]
        part = lambda ref: ref[b, :, first:first + size, :].reshape(heads * size, dim)
        part_t = lambda ref: jnp.concatenate(
            [ref[b, :, g * rows + first:g * rows + first + size] for g in range(heads)], axis=1)
        wide = lambda x: jnp.concatenate([x] * (half // dim), axis=1)
        logits = dot(part(q), kk, NT)
        prob = jnp.exp2(logits * scale2 - wide(part(lseb)))
        if masked:
            row = lax.broadcasted_iota(jnp.int32, prob.shape, 0) & (size - 1)
            col = lax.broadcasted_iota(jnp.int32, prob.shape, 1)
            prob = jnp.where(col <= row, prob, 0.0)
        d_prob = dot(part(do), vv, NT)
        score = (prob * (d_prob - wide(part(delb)))).astype(jnp.bfloat16)
        prob = prob.astype(jnp.bfloat16)
        acc[slot, h, 1] += dot(part_t(dot_t), prob, NN)
        acc[slot, h, 0] += dot(part_t(qt), score, NN)
        dq[b, :, first:first + size, :] += dot(score, kk, NN).reshape(heads, size, dim)

    prep(core)
    tile(core, 0, own_slot + core, 0, True)
    tile(core, 1, own_slot + core, 0, False)

    theirs = [
        remote(kv.at[own_slot + other, 0], kv.at[own_slot + other, 0], pair_send.at[0], pair_recv.at[0], {'cp': partner}),
        remote(kv.at[own_slot + other, 1], kv.at[own_slot + other, 1], pair_send.at[1], pair_recv.at[1], {'cp': partner}),
        remote(q.at[other], q.at[other], pair_send.at[2], pair_recv.at[2], {'cp': partner}),
        remote(do.at[other], do.at[other], pair_send.at[3], pair_recv.at[3], {'cp': partner}),
        remote(ld.at[other], ld.at[other], pair_send.at[4], pair_recv.at[4], {'cp': partner}),
    ]
    for copy in theirs:
        copy.wait_recv()

    @pl.when(late_wrap)
    def _():
        kv_send_own(1, last)

    prep(other)
    tile(other, 1, own_slot + other, 1, True)
    tile(1, None, own_slot, core, False)

    swap = remote(acc.at[own_slot + other, 1], rhalf, d_send.at[0], d_recv.at[0], {'cp': partner})
    swap.start()

    def g_copy(slot, h, buf, to_chip):
        return remote(acc.at[slot, h], rbuf.at[buf, h], g_send.at[slot, h], g_recv.at[buf, h], at(to_chip))

    def g_wait(buf, h):
        g_copy(0, h, buf, chip).wait_recv()

    def add_relayed(slot, h):
        g_wait(R, h)
        acc[slot, h] += rbuf[R, h]

    def send_partial(slot, h):
        @pl.when(jnp.logical_and(chip == 1, core == 1))
        def _():
            g_copy(slot, h, A, 0).start()

        @pl.when(chip == 2)
        def _():
            @pl.when(jnp.logical_and(slot == 1, core == 1))
            def _():
                g_copy(slot, h, A, 1).start()

            @pl.when(jnp.logical_and(slot == 0, core == 0))
            def _():
                g_copy(slot, h, R, 1).start()

            @pl.when(jnp.logical_and(slot == 0, core == 1))
            def _():
                g_copy(slot, h, R, 3).start()

        @pl.when(chip == 3)
        def _():
            @pl.when(jnp.logical_and(slot == 0, core == 0))
            def _():
                g_copy(slot, h, B, 0).start()

            @pl.when(jnp.logical_and(slot == 0, core == 1))
            def _():
                add_relayed(slot, h)
                g_copy(slot, h, B, 0).start()

            @pl.when(jnp.logical_and(slot == 1, core == 0))
            def _():
                g_copy(slot, h, R, 2).start()

            @pl.when(jnp.logical_and(slot == 1, core == 1))
            def _():
                g_copy(slot, h, R, 0).start()

            @pl.when(slot == 2)
            def _():
                g_copy(slot, h, A, 2).start()

    @pl.loop(0, chip)
    def _(t):
        slot = jnp.where(jnp.logical_and(chip == last, core == 0), t, chip - 1 - t)
        for copy in kv_copies(slot, own_slot + core, 0, at(chip)):
            copy.wait_recv()

        @pl.when(jnp.logical_and(chip < last, slot == chip - 1))
        def _():
            for copy in kv_copies(slot, slot, 2, at(chip + 1)):
                copy.start()

            @pl.when(late_next)
            def _():
                kv_send_own(0, chip + 1)

        @pl.loop(0, 2)
        def _(h):
            @pl.loop(0, 2)
            def _(b):
                tile(b, None, slot, h, False)

            send_partial(slot, h)

    give_dq = remote(dq.at[other], rdq, d_send.at[1], d_recv.at[1], {'cp': partner})
    give_dq.start()

    relay_add = jnp.logical_and(jnp.logical_or(chip == 1, chip == 2), core == 0)
    relay_pass = jnp.logical_and(chip == 0, core == 1)

    def pass_copy(h):
        return remote(rbuf.at[R, h], rbuf.at[B, h], f_send.at[h], g_recv.at[B, h], at(1))

    for h in range(2):
        @pl.when(relay_add)
        def _():
            add_relayed(chip - 1, h)
            g_copy(chip - 1, h, A, chip - 1).start()

        @pl.when(relay_pass)
        def _():
            g_wait(R, h)
            pass_copy(h).start()

    give_dq.wait_recv()
    for g in range(heads):
        gq[g] = ((dq[core, g] + rdq[g]) * scale).astype(gq.dtype)

    swap.wait_recv()
    from_b = jnp.logical_or(chip == 0, jnp.logical_and(chip == 1, core == 1))
    for h in range(2):
        if h == 1:
            swap_in = rhalf[...]
            swap.wait_send()
            acc[own_slot + core, 1] = swap_in

        @pl.when(chip < last)
        def _():
            g_wait(A, h)
            acc[own_slot + core, h] += rbuf[A, h]

        @pl.when(from_b)
        def _():
            g_wait(B, h)
            acc[own_slot + core, h] += rbuf[B, h]

        gk[h * half:(h + 1) * half, :] = (acc[own_slot + core, h, 0].T * scale).astype(gk.dtype)
        gv[h * half:(h + 1) * half, :] = acc[own_slot + core, h, 1].T.astype(gv.dtype)

    for copy in pair:
        copy.wait_send()
    give_dq.wait_send()

    @pl.when(chip < last)
    def _():
        kv_wait_sent(0)

    @pl.when(chip == 0)
    def _():
        kv_wait_sent(1)

    @pl.when(jnp.logical_and(chip >= 1, chip < last))
    def _():
        kv_wait_sent(2)

    @pl.loop(0, chip)
    def _(slot):
        for h in range(2):
            g_copy(slot, h, A, chip).wait_send()

    @pl.when(relay_pass)
    def _():
        for h in range(2):
            pass_copy(h).wait_send()


def solution(mesh):
    n_dev = mesh.shape['cp']
    row_spec = P(('dp', 'cp'))

    def local_fn(q_tok, k_tok, v_tok, fwd_out, d_out, lse_row):
        rows, heads, dim = q_tok.shape
        half = rows // 2
        row_delta = jnp.einsum('rgd,rgd->rg', d_out, fwd_out, preferred_element_type=jnp.float32)
        row_data = jnp.concatenate(
            [lse_row * LOG2E, row_delta, jnp.zeros((rows, dim - 2 * heads), jnp.float32)], axis=1)
        n_slot = n_dev // 2 + 2
        bf16, f32 = jnp.bfloat16, jnp.float32
        any_spec = pl.BlockSpec(memory_space=pl.ANY)
        vmem_spec = pl.BlockSpec(memory_space=pltpu.VMEM)
        dma = pltpu.SemaphoreType.DMA
        gq, gk, gv = pl.pallas_call(
            functools.partial(kernel, n_dev),
            out_shape=[
                jax.ShapeDtypeStruct((heads, rows, dim), bf16),
                jax.ShapeDtypeStruct((rows, dim), bf16),
                jax.ShapeDtypeStruct((rows, dim), bf16),
            ],
            in_specs=[any_spec] * 5,
            out_specs=[vmem_spec] * 3,
            scratch_shapes=[
                pltpu.VMEM((2, heads, rows, dim), bf16),
                pltpu.VMEM((2, heads, rows, dim), bf16),
                pltpu.VMEM((2, dim, heads * rows), bf16),
                pltpu.VMEM((2, dim, heads * rows), bf16),
                pltpu.VMEM((2, rows, dim), f32),
                pltpu.VMEM((2, heads, rows, dim), f32),
                pltpu.VMEM((2, heads, rows, dim), f32),
                pltpu.VMEM((n_slot, 2, rows, dim), bf16),
                pltpu.VMEM((n_slot, 2, 2, dim, half), f32),
                pltpu.VMEM((2, heads, rows, dim), f32),
                pltpu.VMEM((3, 2, 2, dim, half), f32),
                pltpu.VMEM((2, dim, half), f32),
                pltpu.VMEM((heads, rows, dim), f32),
                dma((5,)), dma((5,)), dma((5,)),
                dma((3, 2)), dma((n_slot, 2)),
                dma((n_slot, 2)), dma((3, 2)), dma((2,)), dma((2,)), dma((2,)),
            ],
            compiler_params=pltpu.CompilerParams(
                collective_id=0, has_side_effects=True, vmem_limit_bytes=62 * 2 ** 20),
            name='attn_bwd',
        )(q_tok.transpose(1, 0, 2), d_out.transpose(1, 0, 2), row_data, k_tok, v_tok)
        return gq.transpose(1, 0, 2), gk, gv

    return jax.shard_map(local_fn, mesh=mesh, in_specs=(row_spec,) * 6, out_specs=(row_spec,) * 3, check_vma=False)
```

```python
import functools
import math

import jax
import jax.numpy as jnp
from jax import lax
from jax.experimental import pallas as pl
from jax.experimental.pallas import tpu as pltpu
from jax.sharding import PartitionSpec as P

NT = (((1,), (1,)), ((), ()))
NN = (((1,), (0,)), ((), ()))
LOG2E = math.log2(math.e)
A, B, R = 0, 1, 2


def dot(a, b, dims):
    return lax.dot_general(a, b, dims, preferred_element_type=jnp.float32)


def kernel(n_dev, q_hbm, do_hbm, fo_hbm, lse_hbm, k_hbm, v_hbm, out_hbm,
           q, do, fo, lse, qt, dot_t, lseb, delb, kv, acc, dq, rbuf, rhalf, rdq, out,
           in_sem, pair_send, pair_recv, kv_send, kv_recv, g_send, g_recv, f_send, d_send, d_recv, out_sem):
    heads, rows, dim = q.shape[1:]
    half = rows // 2
    scale = dim ** -0.5
    scale2 = scale * LOG2E
    own_slot = n_dev // 2
    n_chip = n_dev // 2

    me = lax.axis_index('cp')
    chip, core = me // 2, me % 2
    other = 1 - core
    partner = chip * 2 + other

    def at(chip_id):
        return {'cp': chip_id * 2 + core}

    loads = [
        pltpu.make_async_copy(k_hbm, kv.at[own_slot + core, 0], in_sem.at[0]),
        pltpu.make_async_copy(v_hbm, kv.at[own_slot + core, 1], in_sem.at[1]),
        pltpu.make_async_copy(q_hbm, q.at[core], in_sem.at[2]),
        pltpu.make_async_copy(do_hbm, do.at[core], in_sem.at[3]),
        pltpu.make_async_copy(fo_hbm, fo.at[core], in_sem.at[4]),
        pltpu.make_async_copy(lse_hbm, lse.at[core], in_sem.at[5]),
    ]
    for copy in loads:
        copy.start()

    barrier = pltpu.get_barrier_semaphore()
    for d in range(1, n_dev):
        pl.semaphore_signal(barrier, inc=1, device_id={'cp': lax.rem(me + d, n_dev)}, device_id_type=pl.DeviceIdType.MESH)
    acc[...] = jnp.zeros_like(acc)
    dq[...] = jnp.zeros_like(dq)
    pl.semaphore_wait(barrier, n_dev - 1)

    def remote(src, dst, send, recv, device):
        return pltpu.make_async_remote_copy(src_ref=src, dst_ref=dst, send_sem=send, recv_sem=recv,
                                            device_id=device, device_id_type=pl.DeviceIdType.MESH)

    def kv_copies(slot, src_slot, sem_row, device):
        return [remote(kv.at[src_slot, i], kv.at[slot, i], kv_send.at[sem_row, i], kv_recv.at[slot, i], device)
                for i in range(2)]

    def kv_send_own(sem_row, to_chip):
        for copy in kv_copies(chip, own_slot + core, sem_row, at(to_chip)):
            copy.start()

    def kv_wait_sent(sem_row):
        for copy in kv_copies(0, 0, sem_row, at(chip)):
            copy.wait_send()

    last = n_chip - 1
    late_next = jnp.logical_and(chip == last - 1, core == 0)
    late_wrap = jnp.logical_and(chip == 0, core == 1)
    loads[0].wait()
    loads[1].wait()

    @pl.when(jnp.logical_and(chip < last, jnp.logical_not(late_next)))
    def _():
        kv_send_own(0, chip + 1)

    @pl.when(jnp.logical_and(chip == 0, core == 0))
    def _():
        kv_send_own(1, last)

    def pair_copies(c):
        refs = (kv.at[own_slot + c, 0], kv.at[own_slot + c, 1], q.at[c], do.at[c], fo.at[c], lse.at[c])
        return [remote(ref, ref, pair_send.at[i], pair_recv.at[i], {'cp': partner}) for i, ref in enumerate(refs)]

    pair = pair_copies(core)
    for i in (2, 3, 4, 5):
        loads[i].wait()
        pair[i].start()
    pair[0].start()
    pair[1].start()

    def prep(b):
        qt[b] = q[b].reshape(heads * rows, dim).T
        dot_t[b] = do[b].reshape(heads * rows, dim).T
        for g in range(heads):
            lseb[b, g] = jnp.broadcast_to(lse[b, g:g + 1, :] * LOG2E, (dim, rows)).T
            delta = jnp.sum(do[b, g].astype(jnp.float32) * fo[b, g].astype(jnp.float32), axis=1, keepdims=True)
            delb[b, g] = jnp.broadcast_to(delta, (rows, dim))

    def tile(b, row_half, slot, h, masked):
        size = rows if row_half is None else half
        first = 0 if row_half is None else row_half * half
        start = pl.multiple_of(h * half, half)
        kk = kv[slot, 0, pl.ds(start, half), :]
        vv = kv[slot, 1, pl.ds(start, half), :]
        part = lambda ref: ref[b, :, first:first + size, :].reshape(heads * size, dim)
        part_t = lambda ref: jnp.concatenate(
            [ref[b, :, g * rows + first:g * rows + first + size] for g in range(heads)], axis=1)
        wide = lambda x: jnp.concatenate([x] * (half // dim), axis=1)
        logits = dot(part(q), kk, NT)
        prob = jnp.exp2(logits * scale2 - wide(part(lseb)))
        if masked:
            row = lax.broadcasted_iota(jnp.int32, prob.shape, 0) & (size - 1)
            col = lax.broadcasted_iota(jnp.int32, prob.shape, 1)
            prob = jnp.where(col <= row, prob, 0.0)
        d_prob = dot(part(do), vv, NT)
        score = (prob * (d_prob - wide(part(delb)))).astype(jnp.bfloat16)
        prob = prob.astype(jnp.bfloat16)
        acc[slot, h, 1] += dot(part_t(dot_t), prob, NN)
        acc[slot, h, 0] += dot(part_t(qt), score, NN)
        dq[b, :, first:first + size, :] += dot(score, kk, NN).reshape(heads, size, dim)

    prep(core)
    tile(core, 0, own_slot + core, 0, True)
    tile(core, 1, own_slot + core, 0, False)

    for copy in pair_copies(other):
        copy.wait_recv()

    @pl.when(late_wrap)
    def _():
        kv_send_own(1, last)

    prep(other)

    def g_copy(slot, h, buf, to_chip):
        return remote(acc.at[slot, h], rbuf.at[buf, h], g_send.at[slot, h], g_recv.at[buf, h], at(to_chip))

    def g_wait(buf, h):
        g_copy(0, h, buf, chip).wait_recv()

    def add_relayed(slot, h):
        g_wait(R, h)
        acc[slot, h] += rbuf[R, h]

    def send_partial(slot, h):
        @pl.when(jnp.logical_and(chip == 1, core == 1))
        def _():
            g_copy(slot, h, A, 0).start()

        @pl.when(chip == 2)
        def _():
            @pl.when(jnp.logical_and(slot == 1, core == 1))
            def _():
                g_copy(slot, h, A, 1).start()

            @pl.when(jnp.logical_and(slot == 0, core == 0))
            def _():
                g_copy(slot, h, R, 1).start()

            @pl.when(jnp.logical_and(slot == 0, core == 1))
            def _():
                g_copy(slot, h, R, 3).start()

        @pl.when(chip == 3)
        def _():
            @pl.when(jnp.logical_and(slot == 0, core == 0))
            def _():
                g_copy(slot, h, B, 0).start()

            @pl.when(jnp.logical_and(slot == 0, core == 1))
            def _():
                add_relayed(slot, h)
                g_copy(slot, h, B, 0).start()

            @pl.when(jnp.logical_and(slot == 1, core == 0))
            def _():
                g_copy(slot, h, R, 2).start()

            @pl.when(jnp.logical_and(slot == 1, core == 1))
            def _():
                g_copy(slot, h, R, 0).start()

            @pl.when(slot == 2)
            def _():
                g_copy(slot, h, A, 2).start()

    @pl.loop(0, chip)
    def _(t):
        slot = jnp.where(jnp.logical_and(chip == last, core == 0), t, chip - 1 - t)
        for copy in kv_copies(slot, own_slot + core, 0, at(chip)):
            copy.wait_recv()

        @pl.when(jnp.logical_and(chip < last, slot == chip - 1))
        def _():
            for copy in kv_copies(slot, slot, 2, at(chip + 1)):
                copy.start()

            @pl.when(late_next)
            def _():
                kv_send_own(0, chip + 1)

        @pl.loop(0, 2)
        def _(h):
            @pl.loop(0, 2)
            def _(b):
                tile(b, None, slot, h, False)

            send_partial(slot, h)

    swap = remote(acc.at[own_slot + other, 1], rhalf, d_send.at[0], d_recv.at[0], {'cp': partner})
    give_dq = remote(dq.at[other], rdq, d_send.at[1], d_recv.at[1], {'cp': partner})
    tile(other, 1, own_slot + other, 1, True)

    @pl.when(core == 0)
    def _():
        swap.start()

    @pl.when(core == 1)
    def _():
        give_dq.start()

    tile(1, None, own_slot, core, False)

    @pl.when(core == 1)
    def _():
        swap.start()

    @pl.when(core == 0)
    def _():
        give_dq.start()

    relay_add = jnp.logical_and(jnp.logical_or(chip == 1, chip == 2), core == 0)
    relay_pass = jnp.logical_and(chip == 0, core == 1)

    def pass_copy(h):
        return remote(rbuf.at[R, h], rbuf.at[B, h], f_send.at[h], g_recv.at[B, h], at(1))

    for h in range(2):
        @pl.when(relay_add)
        def _():
            add_relayed(chip - 1, h)
            g_copy(chip - 1, h, A, chip - 1).start()

        @pl.when(relay_pass)
        def _():
            g_wait(R, h)
            pass_copy(h).start()

    give_dq.wait_recv()
    for g in range(heads):
        out[g] = ((dq[core, g] + rdq[g]) * scale).astype(out.dtype)
    stores = [pltpu.make_async_copy(out.at[0:heads], out_hbm.at[0:heads], out_sem.at[0])]
    for h in range(2):
        span = pl.ds(h * half, half)
        for i in range(2):
            stores.append(pltpu.make_async_copy(
                out.at[heads + i, span], out_hbm.at[heads + i, span], out_sem.at[1 + 2 * h + i]))
    stores[0].start()

    swap.wait_recv()
    from_b = jnp.logical_or(chip == 0, jnp.logical_and(chip == 1, core == 1))
    for h in range(2):
        if h == 1:
            swap_in = rhalf[...]
            swap.wait_send()
            acc[own_slot + core, 1] = swap_in

        @pl.when(chip < last)
        def _():
            g_wait(A, h)
            acc[own_slot + core, h] += rbuf[A, h]

        @pl.when(from_b)
        def _():
            g_wait(B, h)
            acc[own_slot + core, h] += rbuf[B, h]

        out[heads, h * half:(h + 1) * half, :] = (acc[own_slot + core, h, 0].T * scale).astype(out.dtype)
        out[heads + 1, h * half:(h + 1) * half, :] = acc[own_slot + core, h, 1].T.astype(out.dtype)
        stores[1 + 2 * h].start()
        stores[2 + 2 * h].start()

    for copy in pair:
        copy.wait_send()
    give_dq.wait_send()

    @pl.when(chip < last)
    def _():
        kv_wait_sent(0)

    @pl.when(chip == 0)
    def _():
        kv_wait_sent(1)

    @pl.when(jnp.logical_and(chip >= 1, chip < last))
    def _():
        kv_wait_sent(2)

    @pl.loop(0, chip)
    def _(slot):
        for h in range(2):
            g_copy(slot, h, A, chip).wait_send()

    @pl.when(relay_pass)
    def _():
        for h in range(2):
            pass_copy(h).wait_send()

    for copy in stores:
        copy.wait()


def unpack_kernel(packed, gq, gk, gv, held, in_sem, out_sem):
    heads = gq.shape[0]
    n = packed.shape[0]
    reads = [pltpu.make_async_copy(packed.at[i], held.at[i], in_sem.at[i]) for i in range(n)]
    outs = [gq.at[i] for i in range(heads)] + [gk, gv]
    writes = [pltpu.make_async_copy(held.at[i], outs[i], out_sem.at[i]) for i in range(n)]
    for copy in reads:
        copy.start()
    for read, write in zip(reads, writes):
        read.wait()
        write.start()
    for copy in writes:
        copy.wait()


def solution(mesh):
    n_dev = mesh.shape['cp']
    row_spec = P(('dp', 'cp'))

    def local_fn(q_tok, k_tok, v_tok, fwd_out, d_out, lse_row):
        rows, heads, dim = q_tok.shape
        half = rows // 2
        n_slot = n_dev // 2 + 2
        bf16, f32 = jnp.bfloat16, jnp.float32
        any_spec = pl.BlockSpec(memory_space=pl.ANY)
        dma = pltpu.SemaphoreType.DMA
        packed = pl.pallas_call(
            functools.partial(kernel, n_dev),
            out_shape=jax.ShapeDtypeStruct((heads + 2, rows, dim), bf16),
            in_specs=[any_spec] * 6,
            out_specs=any_spec,
            scratch_shapes=[
                pltpu.VMEM((2, heads, rows, dim), bf16),
                pltpu.VMEM((2, heads, rows, dim), bf16),
                pltpu.VMEM((2, heads, rows, dim), bf16),
                pltpu.VMEM((2, heads, rows), f32),
                pltpu.VMEM((2, dim, heads * rows), bf16),
                pltpu.VMEM((2, dim, heads * rows), bf16),
                pltpu.VMEM((2, heads, rows, dim), f32),
                pltpu.VMEM((2, heads, rows, dim), f32),
                pltpu.VMEM((n_slot, 2, rows, dim), bf16),
                pltpu.VMEM((n_slot, 2, 2, dim, half), f32),
                pltpu.VMEM((2, heads, rows, dim), f32),
                pltpu.VMEM((3, 2, 2, dim, half), f32),
                pltpu.VMEM((2, dim, half), f32),
                pltpu.VMEM((heads, rows, dim), f32),
                pltpu.VMEM((heads + 2, rows, dim), bf16),
                dma((6,)), dma((6,)), dma((6,)),
                dma((3, 2)), dma((n_slot, 2)),
                dma((n_slot, 2)), dma((3, 2)), dma((2,)), dma((2,)), dma((2,)), dma((5,)),
            ],
            compiler_params=pltpu.CompilerParams(
                collective_id=0, has_side_effects=True, vmem_limit_bytes=62 * 2 ** 20),
            name='attn_bwd',
        )(q_tok.transpose(1, 0, 2), d_out.transpose(1, 0, 2), fwd_out.transpose(1, 0, 2), lse_row.T, k_tok, v_tok)
        gq, gk, gv = pl.pallas_call(
            unpack_kernel,
            out_shape=[
                jax.ShapeDtypeStruct((heads, rows, dim), bf16),
                jax.ShapeDtypeStruct((rows, dim), bf16),
                jax.ShapeDtypeStruct((rows, dim), bf16),
            ],
            in_specs=[any_spec],
            out_specs=[any_spec] * 3,
            scratch_shapes=[pltpu.VMEM((heads + 2, rows, dim), bf16), dma((heads + 2,)), dma((heads + 2,))],
            name='unpack',
        )(packed)
        return gq.transpose(1, 0, 2), gk, gv

    return jax.shard_map(local_fn, mesh=mesh, in_specs=(row_spec,) * 6, out_specs=(row_spec,) * 3, check_vma=False)
```

```python
import functools
import math

import jax
import jax.numpy as jnp
from jax import lax
from jax.experimental import pallas as pl
from jax.experimental.pallas import tpu as pltpu
from jax.sharding import PartitionSpec as P

NT = (((1,), (1,)), ((), ()))
NN = (((1,), (0,)), ((), ()))
LOG2E = math.log2(math.e)
A, B, R = 0, 1, 2


def dot(a, b, dims):
    return lax.dot_general(a, b, dims, preferred_element_type=jnp.float32)


def kernel(n_dev, q_hbm, do_hbm, fo_hbm, lse_hbm, k_hbm, v_hbm, out_hbm,
           q, do, fo, lse, stats, qt, dot_t, lseb, delb, kv, acc, dq, rbuf, rhalf, rdq, out,
           guest_q, guest_do, guest_stats, guest_qt, guest_dot, guest_lse, guest_del, guest_dq, back_dq,
           in_sem, pair_send, pair_recv, kv_send, kv_recv, g_send, g_recv, f_send, d_send, d_recv,
           guest_send, guest_recv, out_sem):
    heads, rows, dim = q.shape[1:]
    half = rows // 2
    scale = dim ** -0.5
    scale2 = scale * LOG2E
    own_slot = n_dev // 2
    n_chip = n_dev // 2
    last = n_chip - 1

    me = lax.axis_index('cp')
    chip, core = me // 2, me % 2
    other = 1 - core
    partner = {'cp': chip * 2 + other}

    def at(chip_id):
        return {'cp': chip_id * 2 + core}

    loads = [
        pltpu.make_async_copy(k_hbm, kv.at[own_slot + core, 0], in_sem.at[0]),
        pltpu.make_async_copy(v_hbm, kv.at[own_slot + core, 1], in_sem.at[1]),
        pltpu.make_async_copy(q_hbm, q.at[core], in_sem.at[2]),
        pltpu.make_async_copy(do_hbm, do.at[core], in_sem.at[3]),
        pltpu.make_async_copy(fo_hbm, fo, in_sem.at[4]),
        pltpu.make_async_copy(lse_hbm, lse, in_sem.at[5]),
    ]
    for copy in loads:
        copy.start()

    barrier = pltpu.get_barrier_semaphore()
    for d in range(1, n_dev):
        pl.semaphore_signal(barrier, inc=1, device_id={'cp': lax.rem(me + d, n_dev)}, device_id_type=pl.DeviceIdType.MESH)
    acc[...] = jnp.zeros_like(acc)
    dq[...] = jnp.zeros_like(dq)
    pl.semaphore_wait(barrier, n_dev - 1)

    def remote(src, dst, send, recv, device):
        return pltpu.make_async_remote_copy(src_ref=src, dst_ref=dst, send_sem=send, recv_sem=recv,
                                            device_id=device, device_id_type=pl.DeviceIdType.MESH)

    def kv_copies(slot, src_slot, h, sem_row, device):
        span = pl.ds(h * half, half)
        return [remote(kv.at[src_slot, i, span], kv.at[slot, i, span],
                       kv_send.at[sem_row, h, i], kv_recv.at[slot, h, i], device) for i in range(2)]

    def kv_send_own(sem_row, to_chip):
        for h in range(2):
            for copy in kv_copies(chip, own_slot + core, h, sem_row, at(to_chip)):
                copy.start()

    def kv_wait_sent(sem_row):
        for h in range(2):
            for copy in kv_copies(0, 0, h, sem_row, at(chip)):
                copy.wait_send()

    late_next = jnp.logical_and(chip == last - 1, core == 0)
    late_wrap = jnp.logical_and(chip == 0, core == 1)
    loads[0].wait()
    loads[1].wait()

    @pl.when(jnp.logical_and(chip < last, jnp.logical_not(late_next)))
    def _():
        kv_send_own(0, chip + 1)

    @pl.when(jnp.logical_and(chip == 0, core == 0))
    def _():
        kv_send_own(1, last)

    def pair_copies(c):
        refs = (q.at[c], do.at[c], kv.at[own_slot + c, 0], kv.at[own_slot + c, 1], stats.at[c])
        return [remote(ref, ref, pair_send.at[i], pair_recv.at[i], partner) for i, ref in enumerate(refs)]

    guest_rows = pl.ds(half, half)
    guests = [
        remote(q.at[core, :, guest_rows], guest_q, guest_send.at[0], guest_recv.at[0], at(0)),
        remote(do.at[core, :, guest_rows], guest_do, guest_send.at[1], guest_recv.at[1], at(0)),
        remote(stats.at[core, :, guest_rows], guest_stats, guest_send.at[2], guest_recv.at[2], at(0)),
    ]
    guests_back = remote(guest_dq, back_dq, d_send.at[2], d_recv.at[2], at(last))

    pair = pair_copies(core)
    for i in (2, 3):
        loads[i].wait()

        @pl.when(chip == last)
        def _():
            guests[i - 2].start()

        pair[i - 2].start()
    pair[2].start()
    pair[3].start()
    loads[4].wait()
    loads[5].wait()
    for g in range(heads):
        stats[core, g:g + 1, :] = lse[g:g + 1, :] * LOG2E
        product = do[core, g].astype(jnp.float32) * fo[g].astype(jnp.float32)
        stats[core, heads + g:heads + g + 1, :] = jnp.sum(product.T, axis=0, keepdims=True)
    pair[4].start()

    @pl.when(chip == last)
    def _():
        guests[2].start()

    def spread(row):
        return jnp.broadcast_to(row, (dim, row.shape[1])).T

    def prep(b):
        qt[b] = q[b].reshape(heads * rows, dim).T
        dot_t[b] = do[b].reshape(heads * rows, dim).T
        for g in range(heads):
            lseb[b, g] = spread(stats[b, g:g + 1, :])
            delb[b, g] = spread(stats[b, heads + g:heads + g + 1, :])

    def pair_grads(q_rows, do_rows, q_cols, do_cols, lse_rows, del_rows, kk, vv, size, masked):
        wide = lambda x: jnp.concatenate([x] * (kk.shape[0] // dim), axis=1)
        logits = dot(q_rows, kk, NT)
        prob = jnp.exp2(logits * scale2 - wide(lse_rows))
        if masked:
            row = lax.broadcasted_iota(jnp.int32, prob.shape, 0) & (size - 1)
            col = lax.broadcasted_iota(jnp.int32, prob.shape, 1)
            prob = jnp.where(col <= row, prob, 0.0)
        d_prob = dot(do_rows, vv, NT)
        score = (prob * (d_prob - wide(del_rows))).astype(jnp.bfloat16)
        prob = prob.astype(jnp.bfloat16)
        return dot(q_cols, score, NN), dot(do_cols, prob, NN), dot(score, kk, NN)

    def tile(blocks, first, size, slot, h, masked=False):
        start = pl.multiple_of(h * half, half)
        kk = kv[slot, 0, pl.ds(start, half), :]
        vv = kv[slot, 1, pl.ds(start, half), :]
        part = lambda ref: jnp.concatenate(
            [ref[b, :, first:first + size, :].reshape(heads * size, dim) for b in blocks], axis=0)
        part_t = lambda ref: jnp.concatenate(
            [ref[b, :, g * rows + first:g * rows + first + size] for b in blocks for g in range(heads)], axis=1)
        d_key, d_value, d_query = pair_grads(
            part(q), part(do), part_t(qt), part_t(dot_t), part(lseb), part(delb), kk, vv, size, masked)
        acc[slot, h, 0] += d_key
        acc[slot, h, 1] += d_value
        for i, b in enumerate(blocks):
            n = heads * size
            dq[b, :, first:first + size, :] += d_query[i * n:(i + 1) * n].reshape(heads, size, dim)

    prep(core)
    tile((core,), 0, half, own_slot + core, 0, masked=True)
    tile((core,), half, half, own_slot + core, 0)

    for copy in pair_copies(other):
        copy.wait_recv()

    @pl.when(late_wrap)
    def _():
        kv_send_own(1, last)

    prep(other)

    @pl.when(chip == 0)
    def _():
        for copy in guests:
            copy.wait_recv()
        n = heads * half
        guest_qt[...] = guest_q[...].reshape(n, dim).T
        guest_dot[...] = guest_do[...].reshape(n, dim).T
        for g in range(heads):
            guest_lse[g] = spread(guest_stats[g:g + 1, :])
            guest_del[g] = spread(guest_stats[heads + g:heads + g + 1, :])
        guest_dq[...] = jnp.zeros_like(guest_dq)

        @pl.loop(0, 2)
        def _(b):
            flat = lambda ref: ref[...].reshape(n, dim)
            d_key, d_value, d_query = pair_grads(
                flat(guest_q), flat(guest_do), guest_qt[...], guest_dot[...], flat(guest_lse), flat(guest_del),
                kv[own_slot + b, 0], kv[own_slot + b, 1], half, False)
            for h in range(2):
                acc[own_slot + b, h, 0] += d_key[:, h * half:(h + 1) * half]
                acc[own_slot + b, h, 1] += d_value[:, h * half:(h + 1) * half]
            guest_dq[...] += d_query.reshape(heads, half, dim)

        guests_back.start()

    def g_copy(slot, h, buf, to_chip):
        return remote(acc.at[slot, h], rbuf.at[buf, h], g_send.at[slot, h], g_recv.at[buf, h], at(to_chip))

    def g_wait(buf, h):
        g_copy(0, h, buf, chip).wait_recv()

    def add_relayed(slot, h):
        g_wait(R, h)
        acc[slot, h] += rbuf[R, h]

    def send_partial(slot, h):
        @pl.when(jnp.logical_and(chip == 1, core == 1))
        def _():
            g_copy(slot, h, A, 0).start()

        @pl.when(chip == 2)
        def _():
            @pl.when(jnp.logical_and(slot == 1, core == 1))
            def _():
                g_copy(slot, h, A, 1).start()

            @pl.when(jnp.logical_and(slot == 0, core == 0))
            def _():
                g_copy(slot, h, R, 1).start()

            @pl.when(jnp.logical_and(slot == 0, core == 1))
            def _():
                g_copy(slot, h, R, 3).start()

        @pl.when(chip == 3)
        def _():
            @pl.when(jnp.logical_and(slot == 0, core == 0))
            def _():
                g_copy(slot, h, B, 0).start()

            @pl.when(jnp.logical_and(slot == 0, core == 1))
            def _():
                add_relayed(slot, h)
                g_copy(slot, h, B, 0).start()

            @pl.when(jnp.logical_and(slot == 1, core == 0))
            def _():
                g_copy(slot, h, R, 2).start()

            @pl.when(jnp.logical_and(slot == 1, core == 1))
            def _():
                g_copy(slot, h, R, 0).start()

            @pl.when(slot == 2)
            def _():
                g_copy(slot, h, A, 2).start()

    @pl.loop(0, chip)
    def _(t):
        slot = jnp.where(jnp.logical_and(chip == last, core == 0), t, chip - 1 - t)

        @pl.loop(0, 2)
        def _(h):
            for copy in kv_copies(slot, own_slot + core, h, 0, at(chip)):
                copy.wait_recv()

            @pl.when(jnp.logical_and(chip < last, slot == chip - 1))
            def _():
                for copy in kv_copies(slot, slot, h, 2, at(chip + 1)):
                    copy.start()

                @pl.when(jnp.logical_and(late_next, h == 1))
                def _():
                    kv_send_own(0, chip + 1)

            with_guests = jnp.logical_and(chip == last, slot == 0)

            @pl.when(with_guests)
            def _():
                tile((0, 1), 0, half, slot, h)

            @pl.when(jnp.logical_not(with_guests))
            def _():
                @pl.loop(0, 2)
                def _(b):
                    tile((b,), 0, rows, slot, h)

            send_partial(slot, h)

    relay_add = jnp.logical_and(jnp.logical_or(chip == 1, chip == 2), core == 0)
    relay_pass = jnp.logical_and(chip == 0, core == 1)

    def pass_copy(h):
        return remote(rbuf.at[R, h], rbuf.at[B, h], f_send.at[h], g_recv.at[B, h], at(1))

    def relay(h):
        @pl.when(relay_add)
        def _():
            add_relayed(chip - 1, h)
            g_copy(chip - 1, h, A, chip - 1).start()

    swaps = [remote(acc.at[own_slot + other, h], rhalf.at[h], d_send.at[3 * h], d_recv.at[3 * h], partner)
             for h in range(2)]
    give_dq = remote(dq.at[other], rdq, d_send.at[1], d_recv.at[1], partner)

    relay(0)
    tile((other,), half, half, own_slot + other, 1, masked=True)

    @pl.when(core == 0)
    def _():
        swaps[1].start()

    @pl.when(core == 1)
    def _():
        give_dq.start()

    relay(1)
    tile((1,), 0, rows, own_slot, core)

    @pl.when(core == 1)
    def _():
        swaps[1].start()

    @pl.when(core == 0)
    def _():
        give_dq.start()

    @pl.when(chip == 0)
    def _():
        swaps[0].start()

    give_dq.wait_recv()
    for g in range(heads):
        out[g] = ((dq[core, g] + rdq[g]) * scale).astype(out.dtype)

    @pl.when(chip == last)
    def _():
        guests_back.wait_recv()
        for g in range(heads):
            out[g, half:, :] = ((dq[core, g, half:, :] + rdq[g, half:, :] + back_dq[g]) * scale).astype(out.dtype)

    stores = [pltpu.make_async_copy(out.at[0:heads], out_hbm.at[0:heads], out_sem.at[0])]
    for h in range(2):
        span = pl.ds(h * half, half)
        for i in range(2):
            stores.append(pltpu.make_async_copy(
                out.at[heads + i, span], out_hbm.at[heads + i, span], out_sem.at[1 + 2 * h + i]))
    stores[0].start()

    @pl.when(relay_pass)
    def _():
        for h in range(2):
            g_wait(R, h)
            pass_copy(h).start()

    @pl.when(chip == 0)
    def _():
        swaps[0].wait_recv()
        acc[own_slot + core, 0] += rhalf[0]

    swaps[1].wait_recv()
    acc[own_slot + core, 1] += rhalf[1]
    from_b = jnp.logical_or(chip == 0, jnp.logical_and(chip == 1, core == 1))
    for h in range(2):
        @pl.when(chip < last)
        def _():
            g_wait(A, h)
            acc[own_slot + core, h] += rbuf[A, h]

        @pl.when(from_b)
        def _():
            g_wait(B, h)
            acc[own_slot + core, h] += rbuf[B, h]

        out[heads, h * half:(h + 1) * half, :] = (acc[own_slot + core, h, 0].T * scale).astype(out.dtype)
        out[heads + 1, h * half:(h + 1) * half, :] = acc[own_slot + core, h, 1].T.astype(out.dtype)
        stores[1 + 2 * h].start()
        stores[2 + 2 * h].start()

    for copy in pair:
        copy.wait_send()
    give_dq.wait_send()
    swaps[1].wait_send()

    @pl.when(chip == 0)
    def _():
        swaps[0].wait_send()
        guests_back.wait_send()
        kv_wait_sent(1)

    @pl.when(chip == last)
    def _():
        for copy in guests:
            copy.wait_send()

    @pl.when(chip < last)
    def _():
        kv_wait_sent(0)

    @pl.when(jnp.logical_and(chip >= 1, chip < last))
    def _():
        kv_wait_sent(2)

    @pl.loop(0, chip)
    def _(slot):
        for h in range(2):
            g_copy(slot, h, A, chip).wait_send()

    @pl.when(relay_pass)
    def _():
        for h in range(2):
            pass_copy(h).wait_send()

    for copy in stores:
        copy.wait()


def unpack_kernel(packed, gq, gk, gv, held, in_sem, out_sem):
    heads = gq.shape[0]
    n = packed.shape[0]
    reads = [pltpu.make_async_copy(packed.at[i], held.at[i], in_sem.at[i]) for i in range(n)]
    outs = [gq.at[i] for i in range(heads)] + [gk, gv]
    writes = [pltpu.make_async_copy(held.at[i], outs[i], out_sem.at[i]) for i in range(n)]
    for copy in reads:
        copy.start()
    for read, write in zip(reads, writes):
        read.wait()
        write.start()
    for copy in writes:
        copy.wait()


def solution(mesh):
    n_dev = mesh.shape['cp']
    row_spec = P(('dp', 'cp'))

    def local_fn(q_tok, k_tok, v_tok, fwd_out, d_out, lse_row):
        rows, heads, dim = q_tok.shape
        half = rows // 2
        n_slot = n_dev // 2 + 2
        bf16, f32 = jnp.bfloat16, jnp.float32
        any_spec = pl.BlockSpec(memory_space=pl.ANY)
        dma = pltpu.SemaphoreType.DMA
        vmem = pltpu.VMEM
        packed = pl.pallas_call(
            functools.partial(kernel, n_dev),
            out_shape=jax.ShapeDtypeStruct((heads + 2, rows, dim), bf16),
            in_specs=[any_spec] * 6,
            out_specs=any_spec,
            scratch_shapes=[
                vmem((2, heads, rows, dim), bf16), vmem((2, heads, rows, dim), bf16),
                vmem((heads, rows, dim), bf16), vmem((heads, rows), f32), vmem((2, 8, rows), f32),
                vmem((2, dim, heads * rows), bf16), vmem((2, dim, heads * rows), bf16),
                vmem((2, heads, rows, dim), f32), vmem((2, heads, rows, dim), f32),
                vmem((n_slot, 2, rows, dim), bf16),
                vmem((n_slot, 2, 2, dim, half), f32),
                vmem((2, heads, rows, dim), f32),
                vmem((3, 2, 2, dim, half), f32), vmem((2, 2, dim, half), f32),
                vmem((heads, rows, dim), f32),
                vmem((heads + 2, rows, dim), bf16),
                vmem((heads, half, dim), bf16), vmem((heads, half, dim), bf16), vmem((8, half), f32),
                vmem((dim, heads * half), bf16), vmem((dim, heads * half), bf16),
                vmem((heads, half, dim), f32), vmem((heads, half, dim), f32),
                vmem((heads, half, dim), f32), vmem((heads, half, dim), f32),
                dma((6,)), dma((5,)), dma((5,)),
                dma((3, 2, 2)), dma((n_slot, 2, 2)),
                dma((n_slot, 2)), dma((3, 2)), dma((2,)), dma((4,)), dma((4,)),
                dma((3,)), dma((3,)), dma((5,)),
            ],
            compiler_params=pltpu.CompilerParams(
                collective_id=0, has_side_effects=True, vmem_limit_bytes=62 * 2 ** 20),
            name='attn_bwd',
        )(q_tok.transpose(1, 0, 2), d_out.transpose(1, 0, 2), fwd_out.transpose(1, 0, 2), lse_row.T, k_tok, v_tok)
        gq, gk, gv = pl.pallas_call(
            unpack_kernel,
            out_shape=[
                jax.ShapeDtypeStruct((heads, rows, dim), bf16),
                jax.ShapeDtypeStruct((rows, dim), bf16),
                jax.ShapeDtypeStruct((rows, dim), bf16),
            ],
            in_specs=[any_spec],
            out_specs=[any_spec] * 3,
            scratch_shapes=[pltpu.VMEM((heads + 2, rows, dim), bf16), dma((heads + 2,)), dma((heads + 2,))],
            name='unpack',
        )(packed)
        return gq.transpose(1, 0, 2), gk, gv

    return jax.shard_map(local_fn, mesh=mesh, in_specs=(row_spec,) * 6, out_specs=(row_spec,) * 3, check_vma=False)
```

```python
import functools
import math

import jax
import jax.numpy as jnp
from jax import lax
from jax.experimental import pallas as pl
from jax.experimental.pallas import tpu as pltpu
from jax.sharding import PartitionSpec as P

NT = (((1,), (1,)), ((), ()))
NN = (((1,), (0,)), ((), ()))
LOG2E = math.log2(math.e)
A, B, R = 0, 1, 2


def dot(a, b, dims):
    return lax.dot_general(a, b, dims, preferred_element_type=jnp.float32)


def kernel(n_dev, n_guest, q_hbm, do_hbm, fo_hbm, lse_hbm, k_hbm, v_hbm, out_hbm,
           q, do, fo, lse, stats, qt, dot_t, lseb, delb, kv, acc, dq, rbuf, rhalf, rdq, out,
           guest_q, guest_do, guest_stats, guest_qt, guest_dot, guest_lse, guest_del, guest_dq, back_dq,
           in_sem, pair_send, pair_recv, kv_send, kv_recv, g_send, g_recv, f_send, d_send, d_recv,
           guest_send, guest_recv, back_recv, out_sem):
    heads, rows, dim = q.shape[1:]
    half = rows // 2
    scale = dim ** -0.5
    scale2 = scale * LOG2E
    own_slot = n_dev // 2
    n_chip = n_dev // 2
    last = n_chip - 1

    me = lax.axis_index('cp')
    chip, core = me // 2, me % 2
    other = 1 - core
    partner = {'cp': chip * 2 + other}

    def at(chip_id):
        return {'cp': chip_id * 2 + core}

    loads = [
        pltpu.make_async_copy(k_hbm, kv.at[own_slot + core, 0], in_sem.at[0]),
        pltpu.make_async_copy(v_hbm, kv.at[own_slot + core, 1], in_sem.at[1]),
        pltpu.make_async_copy(q_hbm, q.at[core], in_sem.at[2]),
        pltpu.make_async_copy(do_hbm, do.at[core], in_sem.at[3]),
        pltpu.make_async_copy(fo_hbm, fo, in_sem.at[4]),
        pltpu.make_async_copy(lse_hbm, lse, in_sem.at[5]),
    ]
    for copy in loads:
        copy.start()

    barrier = pltpu.get_barrier_semaphore()
    for d in range(1, n_dev):
        pl.semaphore_signal(barrier, inc=1, device_id={'cp': lax.rem(me + d, n_dev)}, device_id_type=pl.DeviceIdType.MESH)
    acc[...] = jnp.zeros_like(acc)
    dq[...] = jnp.zeros_like(dq)
    pl.semaphore_wait(barrier, n_dev - 1)

    def remote(src, dst, send, recv, device):
        return pltpu.make_async_remote_copy(src_ref=src, dst_ref=dst, send_sem=send, recv_sem=recv,
                                            device_id=device, device_id_type=pl.DeviceIdType.MESH)

    def kv_copies(slot, src_slot, h, sem_row, device):
        span = pl.ds(h * half, half)
        return [remote(kv.at[src_slot, i, span], kv.at[slot, i, span],
                       kv_send.at[sem_row, h, i], kv_recv.at[slot, h, i], device) for i in range(2)]

    def give_kv(to_chip, h):
        for copy in kv_copies(chip, own_slot + core, h, to_chip - 1, at(to_chip)):
            copy.start()

    def kv_sent(row):
        for h in range(2):
            for copy in kv_copies(0, 0, h, row, at(chip)):
                copy.wait_send()

    def kv_send_far():
        for h in range(2):
            give_kv(last, h)

    first_far = jnp.logical_or(jnp.logical_and(chip == 0, core == 0), jnp.logical_and(chip == last - 1, core == 1))
    loads[0].wait()
    loads[1].wait()

    @pl.when(first_far)
    def _():
        kv_send_far()

    @pl.when(chip == 0)
    def _():
        for h in range(2):
            give_kv(1, h)

        @pl.when(core == 0)
        def _():
            for h in range(2):
                give_kv(2, h)

    @pl.when(chip == 1)
    def _():
        for h in range(2):
            give_kv(2, h)

    def pair_copies(c):
        refs = (q.at[c], do.at[c], kv.at[own_slot + c, 0], kv.at[own_slot + c, 1], stats.at[c])
        return [remote(ref, ref, pair_send.at[i], pair_recv.at[i], partner) for i, ref in enumerate(refs)]

    def guest_copies(to_chip):
        n = n_guest[to_chip]
        src, dst = pl.ds(rows - n, n), pl.ds(0, n)
        pairs = ((q.at[core, :, src], guest_q.at[:, dst]), (do.at[core, :, src], guest_do.at[:, dst]),
                 (stats.at[core, :, src], guest_stats.at[:, dst]))
        return [remote(src, dst, guest_send.at[to_chip, i], guest_recv.at[i], at(to_chip))
                for i, (src, dst) in enumerate(pairs)]

    guests = [guest_copies(to_chip) for to_chip in range(2)]

    def guests_back(from_chip):
        span = pl.ds(0, n_guest[from_chip])
        return remote(guest_dq.at[:, span], back_dq.at[from_chip, :, span],
                      d_send.at[2], back_recv.at[from_chip], at(last))

    pair = pair_copies(core)
    for i in (2, 3):
        loads[i].wait()

        @pl.when(chip == last)
        def _():
            for copies in guests:
                copies[i - 2].start()

        pair[i - 2].start()
    pair[2].start()
    pair[3].start()
    loads[4].wait()
    loads[5].wait()
    for g in range(heads):
        stats[core, g:g + 1, :] = lse[g:g + 1, :] * LOG2E
        product = do[core, g].astype(jnp.float32) * fo[g].astype(jnp.float32)
        stats[core, heads + g:heads + g + 1, :] = jnp.sum(product.T, axis=0, keepdims=True)
    pair[4].start()

    @pl.when(chip == last)
    def _():
        for copies in guests:
            copies[2].start()

    def spread(row):
        return jnp.broadcast_to(row, (dim, row.shape[1])).T

    def prep(b):
        qt[b] = q[b].reshape(heads * rows, dim).T
        dot_t[b] = do[b].reshape(heads * rows, dim).T
        for g in range(heads):
            lseb[b, g] = spread(stats[b, g:g + 1, :])
            delb[b, g] = spread(stats[b, heads + g:heads + g + 1, :])

    def pair_grads(q_rows, do_rows, q_cols, do_cols, lse_rows, del_rows, kk, vv, size, masked):
        wide = lambda x: jnp.concatenate([x] * (kk.shape[0] // dim), axis=1)
        logits = dot(q_rows, kk, NT)
        prob = jnp.exp2(logits * scale2 - wide(lse_rows))
        if masked:
            row = lax.broadcasted_iota(jnp.int32, prob.shape, 0) & (size - 1)
            col = lax.broadcasted_iota(jnp.int32, prob.shape, 1)
            prob = jnp.where(col <= row, prob, 0.0)
        d_prob = dot(do_rows, vv, NT)
        score = (prob * (d_prob - wide(del_rows))).astype(jnp.bfloat16)
        prob = prob.astype(jnp.bfloat16)
        return dot(q_cols, score, NN), dot(do_cols, prob, NN), dot(score, kk, NN)

    def tile(blocks, first, size, slot, h, masked=False):
        start = pl.multiple_of(h * half, half)
        kk = kv[slot, 0, pl.ds(start, half), :]
        vv = kv[slot, 1, pl.ds(start, half), :]
        part = lambda ref: jnp.concatenate(
            [ref[b, :, first:first + size, :].reshape(heads * size, dim) for b in blocks], axis=0)
        part_t = lambda ref: jnp.concatenate(
            [ref[b, :, g * rows + first:g * rows + first + size] for b in blocks for g in range(heads)], axis=1)
        d_key, d_value, d_query = pair_grads(
            part(q), part(do), part_t(qt), part_t(dot_t), part(lseb), part(delb), kk, vv, size, masked)
        acc[slot, h, 0] += d_key
        acc[slot, h, 1] += d_value
        for i, b in enumerate(blocks):
            n = heads * size
            dq[b, :, first:first + size, :] += d_query[i * n:(i + 1) * n].reshape(heads, size, dim)

    def own_low():
        tile((core,), half, half, own_slot + core, 0)

    def partner_masked():
        tile((other,), half, half, own_slot + other, 1, masked=True)

    def square():
        tile((1,), 0, rows, own_slot, core)

    prep(core)
    tile((core,), 0, half, own_slot + core, 0, masked=True)

    @pl.when(core == 1)
    def _():
        own_low()

    for copy in pair_copies(other):
        copy.wait_recv()

    @pl.when(jnp.logical_and(chip == 0, core == 1))
    def _():
        kv_send_far()

    prep(other)

    @pl.when(core == 0)
    def _():
        partner_masked()

    def host(to_chip):
        for copy in guests[to_chip]:
            copy.wait_recv()
        size = n_guest[to_chip]
        n = heads * size
        flat = lambda ref: ref[:, :size, :].reshape(n, dim)
        guest_qt[:, :n] = flat(guest_q).T
        guest_dot[:, :n] = flat(guest_do).T
        for g in range(heads):
            guest_lse[g, :size] = spread(guest_stats[g:g + 1, :size])
            guest_del[g, :size] = spread(guest_stats[heads + g:heads + g + 1, :size])
        guest_dq[:, :size] = jnp.zeros((heads, size, dim), jnp.float32)

        @pl.loop(0, 2)
        def _(b):
            d_key, d_value, d_query = pair_grads(
                flat(guest_q), flat(guest_do), guest_qt[:, :n], guest_dot[:, :n], flat(guest_lse), flat(guest_del),
                kv[own_slot + b, 0], kv[own_slot + b, 1], size, False)
            for h in range(2):
                acc[own_slot + b, h, 0] += d_key[:, h * half:(h + 1) * half]
                acc[own_slot + b, h, 1] += d_value[:, h * half:(h + 1) * half]
            guest_dq[:, :size] += d_query.reshape(heads, size, dim)

        guests_back(to_chip).start()

    for to_chip in range(2):
        @pl.when(chip == to_chip)
        def _():
            host(to_chip)

    def g_copy(slot, h, buf, to_chip):
        return remote(acc.at[slot, h], rbuf.at[buf, h], g_send.at[slot, h], g_recv.at[buf, h], at(to_chip))

    def g_wait(buf, h):
        g_copy(0, h, buf, chip).wait_recv()

    def add_relayed(slot, h):
        g_wait(R, h)
        acc[slot, h] += rbuf[R, h]

    def send_partial(slot, h):
        @pl.when(jnp.logical_and(chip == 1, core == 1))
        def _():
            g_copy(slot, h, A, 0).start()

        @pl.when(chip == 2)
        def _():
            @pl.when(jnp.logical_and(slot == 1, core == 1))
            def _():
                g_copy(slot, h, A, 1).start()

            @pl.when(jnp.logical_and(slot == 0, core == 0))
            def _():
                g_copy(slot, h, R, 1).start()

            @pl.when(jnp.logical_and(slot == 0, core == 1))
            def _():
                g_copy(slot, h, R, 3).start()

        @pl.when(chip == 3)
        def _():
            @pl.when(jnp.logical_and(slot == 0, core == 0))
            def _():
                g_copy(slot, h, B, 0).start()

            @pl.when(jnp.logical_and(slot == 0, core == 1))
            def _():
                add_relayed(slot, h)
                g_copy(slot, h, B, 0).start()

            @pl.when(jnp.logical_and(slot == 1, core == 0))
            def _():
                g_copy(slot, h, R, 2).start()

            @pl.when(jnp.logical_and(slot == 1, core == 1))
            def _():
                g_copy(slot, h, R, 0).start()

            @pl.when(slot == 2)
            def _():
                g_copy(slot, h, A, 2).start()

    @pl.loop(0, 2 * chip)
    def _(u):
        near_first = jnp.where(jnp.logical_and(chip == last, core == 0), u // 2, chip - 1 - u // 2)
        far_inside = chip == last - 1
        inside = jnp.logical_and(far_inside, core == 0)
        slot = jnp.where(inside, jnp.where(jnp.logical_or(u == 0, u == 3), 1, 0), near_first)
        h = jnp.where(inside, u // 2, u % 2)

        def arrived(from_slot, part):
            for copy in kv_copies(from_slot, own_slot + core, part, 0, at(chip)):
                copy.wait_recv()

        def pass_on(from_slot, part, to_chip):
            for copy in kv_copies(from_slot, from_slot, part, from_slot, at(to_chip)):
                copy.start()

        awaited_before = jnp.logical_and(far_inside, jnp.logical_and(slot == 1, h == 1))

        @pl.when(jnp.logical_and(far_inside, u == 1))
        def _():
            arrived(1, 1)
            pass_on(1, 1, last)

        @pl.when(jnp.logical_not(awaited_before))
        def _():
            arrived(slot, h)

        @pl.when(jnp.logical_and(far_inside, u == 0))
        def _():
            pass_on(1, 0, last)

            @pl.when(core == 0)
            def _():
                kv_send_far()

        @pl.when(jnp.logical_and(chip == 1, core == 1))
        def _():
            pass_on(slot, h, 2)

        without_guests = jnp.logical_and(chip == last, slot < 2)
        for to_chip in range(2):
            @pl.when(jnp.logical_and(chip == last, slot == to_chip))
            def _():
                @pl.loop(0, 2)
                def _(b):
                    tile((b,), 0, rows - n_guest[to_chip], slot, h)

        @pl.when(jnp.logical_not(without_guests))
        def _():
            @pl.loop(0, 2)
            def _(b):
                tile((b,), 0, rows, slot, h)

        send_partial(slot, h)

    relay_add = jnp.logical_and(jnp.logical_or(chip == 1, chip == 2), core == 0)
    relay_pass = jnp.logical_and(chip == 0, core == 1)

    def pass_copy(h):
        return remote(rbuf.at[R, h], rbuf.at[B, h], f_send.at[h], g_recv.at[B, h], at(1))

    def relay(h):
        @pl.when(relay_add)
        def _():
            add_relayed(chip - 1, h)
            g_copy(chip - 1, h, A, chip - 1).start()

    swaps = [remote(acc.at[own_slot + other, h], rhalf.at[h], d_send.at[3 * h], d_recv.at[3 * h], partner)
             for h in range(2)]
    give_dq = remote(dq.at[other], rdq, d_send.at[1], d_recv.at[1], partner)

    relay(0)

    @pl.when(core == 0)
    def _():
        swaps[1].start()
        square()

    @pl.when(core == 1)
    def _():
        partner_masked()

    give_dq.start()
    relay(1)

    @pl.when(core == 0)
    def _():
        own_low()

    @pl.when(core == 1)
    def _():
        square()
        swaps[1].start()

    @pl.when(chip < 2)
    def _():
        swaps[0].start()

    give_dq.wait_recv()
    for g in range(heads):
        out[g] = ((dq[core, g] + rdq[g]) * scale).astype(out.dtype)

    @pl.when(chip == last)
    def _():
        for from_chip in range(2):
            guests_back(from_chip).wait_recv()
        for g in range(heads):
            for n in (n_guest[0], n_guest[1]):
                first = rows - n
                total = dq[core, g, first:, :] + rdq[g, first:, :] + back_dq[0, g, n_guest[0] - n:, :]
                if n == n_guest[1]:
                    total = total + back_dq[1, g, :n, :]
                out[g, first:, :] = (total * scale).astype(out.dtype)

    stores = [pltpu.make_async_copy(out.at[0:heads], out_hbm.at[0:heads], out_sem.at[0])]
    for h in range(2):
        span = pl.ds(h * half, half)
        for i in range(2):
            stores.append(pltpu.make_async_copy(
                out.at[heads + i, span], out_hbm.at[heads + i, span], out_sem.at[1 + 2 * h + i]))
    stores[0].start()

    @pl.when(relay_pass)
    def _():
        for h in range(2):
            g_wait(R, h)
            pass_copy(h).start()

    @pl.when(chip < 2)
    def _():
        swaps[0].wait_recv()
        acc[own_slot + core, 0] += rhalf[0]

    swaps[1].wait_recv()
    acc[own_slot + core, 1] += rhalf[1]
    from_b = jnp.logical_or(chip == 0, jnp.logical_and(chip == 1, core == 1))
    for h in range(2):
        @pl.when(chip < last)
        def _():
            g_wait(A, h)
            acc[own_slot + core, h] += rbuf[A, h]

        @pl.when(from_b)
        def _():
            g_wait(B, h)
            acc[own_slot + core, h] += rbuf[B, h]

        out[heads, h * half:(h + 1) * half, :] = (acc[own_slot + core, h, 0].T * scale).astype(out.dtype)
        out[heads + 1, h * half:(h + 1) * half, :] = acc[own_slot + core, h, 1].T.astype(out.dtype)
        stores[1 + 2 * h].start()
        stores[2 + 2 * h].start()

    for copy in pair:
        copy.wait_send()
    give_dq.wait_send()
    swaps[1].wait_send()

    @pl.when(chip < 2)
    def _():
        swaps[0].wait_send()

    for from_chip in range(2):
        @pl.when(chip == from_chip)
        def _():
            guests_back(from_chip).wait_send()

    @pl.when(chip == last)
    def _():
        for copies in guests:
            for copy in copies:
                copy.wait_send()

    @pl.when(jnp.logical_or(chip == 0, chip == last - 1))
    def _():
        kv_sent(last - 1)

    @pl.when(jnp.logical_and(chip < last, me != 1))
    def _():
        kv_sent(1)

    @pl.when(jnp.logical_or(chip == 0, me == 3))
    def _():
        kv_sent(0)

    @pl.loop(0, chip)
    def _(slot):
        for h in range(2):
            g_copy(slot, h, A, chip).wait_send()

    @pl.when(relay_pass)
    def _():
        for h in range(2):
            pass_copy(h).wait_send()

    for copy in stores:
        copy.wait()


def unpack_kernel(packed, gq, gk, gv, held, in_sem, out_sem):
    heads = gq.shape[0]
    n = packed.shape[0]
    reads = [pltpu.make_async_copy(packed.at[i], held.at[i], in_sem.at[i]) for i in range(n)]
    outs = [gq.at[i] for i in range(heads)] + [gk, gv]
    writes = [pltpu.make_async_copy(held.at[i], outs[i], out_sem.at[i]) for i in range(n)]
    for copy in reads:
        copy.start()
    for read, write in zip(reads, writes):
        read.wait()
        write.start()
    for copy in writes:
        copy.wait()


def solution(mesh):
    n_dev = mesh.shape['cp']
    row_spec = P(('dp', 'cp'))

    def local_fn(q_tok, k_tok, v_tok, fwd_out, d_out, lse_row):
        rows, heads, dim = q_tok.shape
        half = rows // 2
        n_guest = (3 * rows // 8, rows // 4)
        most = max(n_guest)
        n_slot = n_dev // 2 + 2
        bf16, f32 = jnp.bfloat16, jnp.float32
        any_spec = pl.BlockSpec(memory_space=pl.ANY)
        dma = pltpu.SemaphoreType.DMA
        vmem = pltpu.VMEM
        packed = pl.pallas_call(
            functools.partial(kernel, n_dev, n_guest),
            out_shape=jax.ShapeDtypeStruct((heads + 2, rows, dim), bf16),
            in_specs=[any_spec] * 6,
            out_specs=any_spec,
            scratch_shapes=[
                vmem((2, heads, rows, dim), bf16), vmem((2, heads, rows, dim), bf16),
                vmem((heads, rows, dim), bf16), vmem((heads, rows), f32), vmem((2, 8, rows), f32),
                vmem((2, dim, heads * rows), bf16), vmem((2, dim, heads * rows), bf16),
                vmem((2, heads, rows, dim), f32), vmem((2, heads, rows, dim), f32),
                vmem((n_slot, 2, rows, dim), bf16),
                vmem((n_slot, 2, 2, dim, half), f32),
                vmem((2, heads, rows, dim), f32),
                vmem((3, 2, 2, dim, half), f32), vmem((2, 2, dim, half), f32),
                vmem((heads, rows, dim), f32),
                vmem((heads + 2, rows, dim), bf16),
                vmem((heads, most, dim), bf16), vmem((heads, most, dim), bf16), vmem((8, most), f32),
                vmem((dim, heads * most), bf16), vmem((dim, heads * most), bf16),
                vmem((heads, most, dim), f32), vmem((heads, most, dim), f32),
                vmem((heads, most, dim), f32), vmem((2, heads, most, dim), f32),
                dma((6,)), dma((5,)), dma((5,)),
                dma((3, 2, 2)), dma((n_slot, 2, 2)),
                dma((n_slot, 2)), dma((3, 2)), dma((2,)), dma((4,)), dma((4,)),
                dma((2, 3)), dma((3,)), dma((2,)), dma((5,)),
            ],
            compiler_params=pltpu.CompilerParams(
                collective_id=0, has_side_effects=True, vmem_limit_bytes=62 * 2 ** 20),
            name='attn_bwd',
        )(q_tok.transpose(1, 0, 2), d_out.transpose(1, 0, 2), fwd_out.transpose(1, 0, 2), lse_row.T, k_tok, v_tok)
        gq, gk, gv = pl.pallas_call(
            unpack_kernel,
            out_shape=[
                jax.ShapeDtypeStruct((heads, rows, dim), bf16),
                jax.ShapeDtypeStruct((rows, dim), bf16),
                jax.ShapeDtypeStruct((rows, dim), bf16),
            ],
            in_specs=[any_spec],
            out_specs=[any_spec] * 3,
            scratch_shapes=[pltpu.VMEM((heads + 2, rows, dim), bf16), dma((heads + 2,)), dma((heads + 2,))],
            name='unpack',
        )(packed)
        return gq.transpose(1, 0, 2), gk, gv

    return jax.shard_map(local_fn, mesh=mesh, in_specs=(row_spec,) * 6, out_specs=(row_spec,) * 3, check_vma=False)
```

```python
import functools
import math

import jax
import jax.numpy as jnp
from jax import lax
from jax.experimental import pallas as pl
from jax.experimental.pallas import tpu as pltpu
from jax.sharding import PartitionSpec as P

NT = (((1,), (1,)), ((), ()))
NN = (((1,), (0,)), ((), ()))
LOG2E = math.log2(math.e)
A, B, R = 0, 1, 2


def dot(a, b, dims):
    return lax.dot_general(a, b, dims, preferred_element_type=jnp.float32)


def kernel(n_dev, n_guest, q_hbm, do_hbm, fo_hbm, lse_hbm, k_hbm, v_hbm, out,
           q, do, fo, lse, stats, qt, dot_t, lseb, delb, kv, acc, dq, rbuf, rhalf, rdq,
           guest_q, guest_do, guest_stats, guest_qt, guest_dot, guest_lse, guest_del, guest_dq, back_dq,
           in_sem, pair_send, pair_recv, kv_send, kv_recv, g_send, g_recv, f_send, d_send, d_recv,
           guest_send, guest_recv, back_recv):
    heads, rows, dim = q.shape[1:]
    half = rows // 2
    scale = dim ** -0.5
    scale2 = scale * LOG2E
    own_slot = n_dev // 2
    n_chip = n_dev // 2
    last = n_chip - 1

    me = lax.axis_index('cp')
    chip, core = me // 2, me % 2
    other = 1 - core
    partner = {'cp': chip * 2 + other}

    def at(chip_id):
        return {'cp': chip_id * 2 + core}

    loads = [
        pltpu.make_async_copy(k_hbm, kv.at[own_slot + core, 0], in_sem.at[0]),
        pltpu.make_async_copy(v_hbm, kv.at[own_slot + core, 1], in_sem.at[1]),
        pltpu.make_async_copy(q_hbm, q.at[core], in_sem.at[2]),
        pltpu.make_async_copy(do_hbm, do.at[core], in_sem.at[3]),
        pltpu.make_async_copy(fo_hbm, fo, in_sem.at[4]),
        pltpu.make_async_copy(lse_hbm, lse, in_sem.at[5]),
    ]
    for copy in loads:
        copy.start()

    barrier = pltpu.get_barrier_semaphore()
    for d in range(1, n_dev):
        pl.semaphore_signal(barrier, inc=1, device_id={'cp': lax.rem(me + d, n_dev)}, device_id_type=pl.DeviceIdType.MESH)
    acc[...] = jnp.zeros_like(acc)
    dq[...] = jnp.zeros_like(dq)
    pl.semaphore_wait(barrier, n_dev - 1)

    def remote(src, dst, send, recv, device):
        return pltpu.make_async_remote_copy(src_ref=src, dst_ref=dst, send_sem=send, recv_sem=recv,
                                            device_id=device, device_id_type=pl.DeviceIdType.MESH)

    def kv_copies(slot, src_slot, h, sem_row, device):
        span = pl.ds(h * half, half)
        return [remote(kv.at[src_slot, i, span], kv.at[slot, i, span],
                       kv_send.at[sem_row, h, i], kv_recv.at[slot, h, i], device) for i in range(2)]

    def give_kv(to_chip, h):
        for copy in kv_copies(chip, own_slot + core, h, to_chip - 1, at(to_chip)):
            copy.start()

    def kv_sent(row):
        for h in range(2):
            for copy in kv_copies(0, 0, h, row, at(chip)):
                copy.wait_send()

    def kv_send_far():
        for h in range(2):
            give_kv(last, h)

    first_far = jnp.logical_or(jnp.logical_and(chip == 0, core == 0), jnp.logical_and(chip == last - 1, core == 1))
    loads[0].wait()
    loads[1].wait()

    @pl.when(first_far)
    def _():
        kv_send_far()

    @pl.when(chip == 0)
    def _():
        for h in range(2):
            give_kv(1, h)

        @pl.when(core == 0)
        def _():
            for h in range(2):
                give_kv(2, h)

    @pl.when(chip == 1)
    def _():
        for h in range(2):
            give_kv(2, h)

    def pair_copies(c):
        refs = (q.at[c], do.at[c], kv.at[own_slot + c, 0], kv.at[own_slot + c, 1], stats.at[c])
        return [remote(ref, ref, pair_send.at[i], pair_recv.at[i], partner) for i, ref in enumerate(refs)]

    def guest_copies(to_chip):
        n = n_guest[to_chip]
        src, dst = pl.ds(rows - n, n), pl.ds(0, n)
        pairs = ((q.at[core, :, src], guest_q.at[:, dst]), (do.at[core, :, src], guest_do.at[:, dst]),
                 (stats.at[core, :, src], guest_stats.at[:, dst]))
        return [remote(src, dst, guest_send.at[to_chip, i], guest_recv.at[i], at(to_chip))
                for i, (src, dst) in enumerate(pairs)]

    guests = [guest_copies(to_chip) for to_chip in range(2)]

    def guests_back(from_chip):
        span = pl.ds(0, n_guest[from_chip])
        return remote(guest_dq.at[:, span], back_dq.at[from_chip, :, span],
                      d_send.at[2], back_recv.at[from_chip], at(last))

    pair = pair_copies(core)
    for i in (2, 3):
        loads[i].wait()

        @pl.when(chip == last)
        def _():
            for copies in guests:
                copies[i - 2].start()

        pair[i - 2].start()
    pair[2].start()
    pair[3].start()
    loads[4].wait()
    loads[5].wait()
    for g in range(heads):
        stats[core, g:g + 1, :] = lse[g:g + 1, :] * LOG2E
        product = do[core, g].astype(jnp.float32) * fo[g].astype(jnp.float32)
        stats[core, heads + g:heads + g + 1, :] = jnp.sum(product.T, axis=0, keepdims=True)
    pair[4].start()

    @pl.when(chip == last)
    def _():
        for copies in guests:
            copies[2].start()

    def spread(row):
        return jnp.broadcast_to(row, (dim, row.shape[1])).T

    def prep(b):
        qt[b] = q[b].reshape(heads * rows, dim).T
        dot_t[b] = do[b].reshape(heads * rows, dim).T
        for g in range(heads):
            lseb[b, g] = spread(stats[b, g:g + 1, :])
            delb[b, g] = spread(stats[b, heads + g:heads + g + 1, :])

    def pair_grads(q_rows, do_rows, q_cols, do_cols, lse_rows, del_rows, kk, vv, size, masked):
        wide = lambda x: jnp.concatenate([x] * (kk.shape[0] // dim), axis=1)
        logits = dot(q_rows, kk, NT)
        prob = jnp.exp2(logits * scale2 - wide(lse_rows))
        if masked:
            row = lax.broadcasted_iota(jnp.int32, prob.shape, 0) & (size - 1)
            col = lax.broadcasted_iota(jnp.int32, prob.shape, 1)
            prob = jnp.where(col <= row, prob, 0.0)
        d_prob = dot(do_rows, vv, NT)
        score = (prob * (d_prob - wide(del_rows))).astype(jnp.bfloat16)
        prob = prob.astype(jnp.bfloat16)
        return dot(q_cols, score, NN), dot(do_cols, prob, NN), dot(score, kk, NN)

    def tile(blocks, first, size, slot, h, masked=False):
        start = pl.multiple_of(h * half, half)
        kk = kv[slot, 0, pl.ds(start, half), :]
        vv = kv[slot, 1, pl.ds(start, half), :]
        part = lambda ref: jnp.concatenate(
            [ref[b, :, first:first + size, :].reshape(heads * size, dim) for b in blocks], axis=0)
        part_t = lambda ref: jnp.concatenate(
            [ref[b, :, g * rows + first:g * rows + first + size] for b in blocks for g in range(heads)], axis=1)
        d_key, d_value, d_query = pair_grads(
            part(q), part(do), part_t(qt), part_t(dot_t), part(lseb), part(delb), kk, vv, size, masked)
        acc[slot, h, 0] += d_key
        acc[slot, h, 1] += d_value
        for i, b in enumerate(blocks):
            n = heads * size
            dq[b, :, first:first + size, :] += d_query[i * n:(i + 1) * n].reshape(heads, size, dim)

    def own_low():
        tile((core,), half, half, own_slot + core, 0)

    def partner_masked():
        tile((other,), half, half, own_slot + other, 1, masked=True)

    def square():
        tile((1,), 0, rows, own_slot, core)

    prep(core)
    tile((core,), 0, half, own_slot + core, 0, masked=True)

    @pl.when(core == 1)
    def _():
        own_low()

    for copy in pair_copies(other):
        copy.wait_recv()

    @pl.when(jnp.logical_and(chip == 0, core == 1))
    def _():
        kv_send_far()

    prep(other)

    @pl.when(core == 0)
    def _():
        partner_masked()

    def host(to_chip):
        for copy in guests[to_chip]:
            copy.wait_recv()
        size = n_guest[to_chip]
        n = heads * size
        flat = lambda ref: ref[:, :size, :].reshape(n, dim)
        guest_qt[:, :n] = flat(guest_q).T
        guest_dot[:, :n] = flat(guest_do).T
        for g in range(heads):
            guest_lse[g, :size] = spread(guest_stats[g:g + 1, :size])
            guest_del[g, :size] = spread(guest_stats[heads + g:heads + g + 1, :size])
        guest_dq[:, :size] = jnp.zeros((heads, size, dim), jnp.float32)

        @pl.loop(0, 2)
        def _(b):
            d_key, d_value, d_query = pair_grads(
                flat(guest_q), flat(guest_do), guest_qt[:, :n], guest_dot[:, :n], flat(guest_lse), flat(guest_del),
                kv[own_slot + b, 0], kv[own_slot + b, 1], size, False)
            for h in range(2):
                acc[own_slot + b, h, 0] += d_key[:, h * half:(h + 1) * half]
                acc[own_slot + b, h, 1] += d_value[:, h * half:(h + 1) * half]
            guest_dq[:, :size] += d_query.reshape(heads, size, dim)

        guests_back(to_chip).start()

    for to_chip in range(2):
        @pl.when(chip == to_chip)
        def _():
            host(to_chip)

    def g_copy(slot, h, buf, to_chip):
        return remote(acc.at[slot, h], rbuf.at[buf, h], g_send.at[slot, h], g_recv.at[buf, h], at(to_chip))

    def g_wait(buf, h):
        g_copy(0, h, buf, chip).wait_recv()

    def add_relayed(slot, h):
        g_wait(R, h)
        acc[slot, h] += rbuf[R, h]

    def send_partial(slot, h):
        @pl.when(jnp.logical_and(chip == 1, core == 1))
        def _():
            g_copy(slot, h, A, 0).start()

        @pl.when(chip == 2)
        def _():
            @pl.when(jnp.logical_and(slot == 1, core == 1))
            def _():
                g_copy(slot, h, A, 1).start()

            @pl.when(jnp.logical_and(slot == 0, core == 0))
            def _():
                g_copy(slot, h, R, 1).start()

            @pl.when(jnp.logical_and(slot == 0, core == 1))
            def _():
                g_copy(slot, h, R, 3).start()

        @pl.when(chip == 3)
        def _():
            @pl.when(jnp.logical_and(slot == 0, core == 0))
            def _():
                g_copy(slot, h, B, 0).start()

            @pl.when(jnp.logical_and(slot == 0, core == 1))
            def _():
                add_relayed(slot, h)
                g_copy(slot, h, B, 0).start()

            @pl.when(jnp.logical_and(slot == 1, core == 0))
            def _():
                g_copy(slot, h, R, 2).start()

            @pl.when(jnp.logical_and(slot == 1, core == 1))
            def _():
                g_copy(slot, h, R, 0).start()

            @pl.when(slot == 2)
            def _():
                g_copy(slot, h, A, 2).start()

    @pl.loop(0, 2 * chip)
    def _(u):
        near_first = jnp.where(jnp.logical_and(chip == last, core == 0), u // 2, chip - 1 - u // 2)
        far_inside = chip == last - 1
        inside = jnp.logical_and(far_inside, core == 0)
        slot = jnp.where(inside, jnp.where(jnp.logical_or(u == 0, u == 3), 1, 0), near_first)
        h = jnp.where(inside, u // 2, u % 2)

        def arrived(from_slot, part):
            for copy in kv_copies(from_slot, own_slot + core, part, 0, at(chip)):
                copy.wait_recv()

        def pass_on(from_slot, part, to_chip):
            for copy in kv_copies(from_slot, from_slot, part, from_slot, at(to_chip)):
                copy.start()

        awaited_before = jnp.logical_and(far_inside, jnp.logical_and(slot == 1, h == 1))

        @pl.when(jnp.logical_and(far_inside, u == 1))
        def _():
            arrived(1, 1)
            pass_on(1, 1, last)

        @pl.when(jnp.logical_not(awaited_before))
        def _():
            arrived(slot, h)

        @pl.when(jnp.logical_and(far_inside, u == 0))
        def _():
            pass_on(1, 0, last)

            @pl.when(core == 0)
            def _():
                kv_send_far()

        @pl.when(jnp.logical_and(chip == 1, core == 1))
        def _():
            pass_on(slot, h, 2)

        without_guests = jnp.logical_and(chip == last, slot < 2)
        for to_chip in range(2):
            @pl.when(jnp.logical_and(chip == last, slot == to_chip))
            def _():
                @pl.loop(0, 2)
                def _(b):
                    tile((b,), 0, rows - n_guest[to_chip], slot, h)

        @pl.when(jnp.logical_not(without_guests))
        def _():
            @pl.loop(0, 2)
            def _(b):
                tile((b,), 0, rows, slot, h)

        send_partial(slot, h)

    relay_add = jnp.logical_and(jnp.logical_or(chip == 1, chip == 2), core == 0)
    relay_pass = jnp.logical_and(chip == 0, core == 1)

    def pass_copy(h):
        return remote(rbuf.at[R, h], rbuf.at[B, h], f_send.at[h], g_recv.at[B, h], at(1))

    def relay(h):
        @pl.when(relay_add)
        def _():
            add_relayed(chip - 1, h)
            g_copy(chip - 1, h, A, chip - 1).start()

    swaps = [remote(acc.at[own_slot + other, h], rhalf.at[h], d_send.at[3 * h], d_recv.at[3 * h], partner)
             for h in range(2)]
    give_dq = remote(dq.at[other], rdq, d_send.at[1], d_recv.at[1], partner)

    relay(0)

    @pl.when(core == 0)
    def _():
        swaps[1].start()
        square()

    @pl.when(core == 1)
    def _():
        partner_masked()

    give_dq.start()
    relay(1)

    @pl.when(core == 0)
    def _():
        own_low()

    @pl.when(core == 1)
    def _():
        square()
        swaps[1].start()

    @pl.when(chip < 2)
    def _():
        swaps[0].start()

    give_dq.wait_recv()
    for g in range(heads):
        out[g] = ((dq[core, g] + rdq[g]) * scale).astype(out.dtype)

    @pl.when(chip == last)
    def _():
        for from_chip in range(2):
            guests_back(from_chip).wait_recv()
        for g in range(heads):
            for n in (n_guest[0], n_guest[1]):
                first = rows - n
                total = dq[core, g, first:, :] + rdq[g, first:, :] + back_dq[0, g, n_guest[0] - n:, :]
                if n == n_guest[1]:
                    total = total + back_dq[1, g, :n, :]
                out[g, first:, :] = (total * scale).astype(out.dtype)

    @pl.when(relay_pass)
    def _():
        for h in range(2):
            g_wait(R, h)
            pass_copy(h).start()

    @pl.when(chip < 2)
    def _():
        swaps[0].wait_recv()
        acc[own_slot + core, 0] += rhalf[0]

    swaps[1].wait_recv()
    acc[own_slot + core, 1] += rhalf[1]
    from_b = jnp.logical_or(chip == 0, jnp.logical_and(chip == 1, core == 1))
    for h in range(2):
        @pl.when(chip < last)
        def _():
            g_wait(A, h)
            acc[own_slot + core, h] += rbuf[A, h]

        @pl.when(from_b)
        def _():
            g_wait(B, h)
            acc[own_slot + core, h] += rbuf[B, h]

        out[heads, h * half:(h + 1) * half, :] = (acc[own_slot + core, h, 0].T * scale).astype(out.dtype)
        out[heads + 1, h * half:(h + 1) * half, :] = acc[own_slot + core, h, 1].T.astype(out.dtype)

    for copy in pair:
        copy.wait_send()
    give_dq.wait_send()
    swaps[1].wait_send()

    @pl.when(chip < 2)
    def _():
        swaps[0].wait_send()

    for from_chip in range(2):
        @pl.when(chip == from_chip)
        def _():
            guests_back(from_chip).wait_send()

    @pl.when(chip == last)
    def _():
        for copies in guests:
            for copy in copies:
                copy.wait_send()

    @pl.when(jnp.logical_or(chip == 0, chip == last - 1))
    def _():
        kv_sent(last - 1)

    @pl.when(jnp.logical_and(chip < last, me != 1))
    def _():
        kv_sent(1)

    @pl.when(jnp.logical_or(chip == 0, me == 3))
    def _():
        kv_sent(0)

    @pl.loop(0, chip)
    def _(slot):
        for h in range(2):
            g_copy(slot, h, A, chip).wait_send()

    @pl.when(relay_pass)
    def _():
        for h in range(2):
            pass_copy(h).wait_send()


def unpack_kernel(packed, gq, gk, gv, out_sem):
    heads = gq.shape[0]
    outs = [gq, gk, gv]
    parts = [packed.at[0:heads], packed.at[heads], packed.at[heads + 1]]
    writes = [pltpu.make_async_copy(part, dst, out_sem.at[i]) for i, (part, dst) in enumerate(zip(parts, outs))]
    for copy in writes:
        copy.start()
    for copy in writes:
        copy.wait()


def solution(mesh):
    n_dev = mesh.shape['cp']
    row_spec = P(('dp', 'cp'))

    def local_fn(q_tok, k_tok, v_tok, fwd_out, d_out, lse_row):
        rows, heads, dim = q_tok.shape
        half = rows // 2
        n_guest = (3 * rows // 8, rows // 4)
        most = max(n_guest)
        n_slot = n_dev // 2 + 2
        bf16, f32 = jnp.bfloat16, jnp.float32
        any_spec = pl.BlockSpec(memory_space=pl.ANY)
        dma = pltpu.SemaphoreType.DMA
        vmem = pltpu.VMEM
        packed = pl.pallas_call(
            functools.partial(kernel, n_dev, n_guest),
            out_shape=vmem((heads + 2, rows, dim), bf16),
            in_specs=[any_spec] * 6,
            out_specs=pl.BlockSpec(memory_space=vmem),
            scratch_shapes=[
                vmem((2, heads, rows, dim), bf16), vmem((2, heads, rows, dim), bf16),
                vmem((heads, rows, dim), bf16), vmem((heads, rows), f32), vmem((2, 8, rows), f32),
                vmem((2, dim, heads * rows), bf16), vmem((2, dim, heads * rows), bf16),
                vmem((2, heads, rows, dim), f32), vmem((2, heads, rows, dim), f32),
                vmem((n_slot, 2, rows, dim), bf16),
                vmem((n_slot, 2, 2, dim, half), f32),
                vmem((2, heads, rows, dim), f32),
                vmem((3, 2, 2, dim, half), f32), vmem((2, 2, dim, half), f32),
                vmem((heads, rows, dim), f32),
                vmem((heads, most, dim), bf16), vmem((heads, most, dim), bf16), vmem((8, most), f32),
                vmem((dim, heads * most), bf16), vmem((dim, heads * most), bf16),
                vmem((heads, most, dim), f32), vmem((heads, most, dim), f32),
                vmem((heads, most, dim), f32), vmem((2, heads, most, dim), f32),
                dma((6,)), dma((5,)), dma((5,)),
                dma((3, 2, 2)), dma((n_slot, 2, 2)),
                dma((n_slot, 2)), dma((3, 2)), dma((2,)), dma((4,)), dma((4,)),
                dma((2, 3)), dma((3,)), dma((2,)),
            ],
            compiler_params=pltpu.CompilerParams(
                collective_id=0, has_side_effects=True, vmem_limit_bytes=56 * 2 ** 20),
            name='attn_bwd',
        )(q_tok.transpose(1, 0, 2), d_out.transpose(1, 0, 2), fwd_out.transpose(1, 0, 2), lse_row.T, k_tok, v_tok)
        gq, gk, gv = pl.pallas_call(
            unpack_kernel,
            out_shape=[
                jax.ShapeDtypeStruct((heads, rows, dim), bf16),
                jax.ShapeDtypeStruct((rows, dim), bf16),
                jax.ShapeDtypeStruct((rows, dim), bf16),
            ],
            in_specs=[pl.BlockSpec(memory_space=vmem)],
            out_specs=[any_spec] * 3,
            scratch_shapes=[dma((3,))],
            name='unpack',
        )(pltpu.with_memory_space_constraint(packed, pltpu.VMEM))
        return gq.transpose(1, 0, 2), gk, gv

    return jax.shard_map(local_fn, mesh=mesh, in_specs=(row_spec,) * 6, out_specs=(row_spec,) * 3, check_vma=False)
```

```python
import functools
import math

import jax
import jax.numpy as jnp
from jax import lax
from jax.experimental import pallas as pl
from jax.experimental.pallas import tpu as pltpu
from jax.sharding import PartitionSpec as P

NT = (((1,), (1,)), ((), ()))
NN = (((1,), (0,)), ((), ()))
LOG2E = math.log2(math.e)
A, B, R = 0, 1, 2


def dot(a, b, dims):
    return lax.dot_general(a, b, dims, preferred_element_type=jnp.float32)


def kernel(n_dev, n_guest, q_hbm, do_hbm, fo_hbm, lse_hbm, k_hbm, v_hbm, out,
           q, do, fo, lse, stats, qt, dot_t, lseb, delb, kv, acc, dq, rbuf, rhalf, rdq,
           guest_q, guest_do, guest_stats, guest_qt, guest_dot, guest_lse, guest_del, guest_dq, back_dq,
           in_sem, pair_send, pair_recv, kv_send, kv_recv, g_send, g_recv, f_send, d_send, d_recv,
           guest_send, guest_recv, back_recv):
    heads, rows, dim = q.shape[1:]
    half = rows // 2
    scale = dim ** -0.5
    scale2 = scale * LOG2E
    own_slot = n_dev // 2
    n_chip = n_dev // 2
    last = n_chip - 1

    me = lax.axis_index('cp')
    chip, core = me // 2, me % 2
    other = 1 - core
    partner = {'cp': chip * 2 + other}

    def at(chip_id):
        return {'cp': chip_id * 2 + core}

    loads = [
        pltpu.make_async_copy(k_hbm, kv.at[own_slot + core, 0], in_sem.at[0]),
        pltpu.make_async_copy(v_hbm, kv.at[own_slot + core, 1], in_sem.at[1]),
        pltpu.make_async_copy(q_hbm, q.at[core], in_sem.at[2]),
        pltpu.make_async_copy(do_hbm, do.at[core], in_sem.at[3]),
        pltpu.make_async_copy(fo_hbm, fo, in_sem.at[4]),
        pltpu.make_async_copy(lse_hbm, lse, in_sem.at[5]),
    ]
    for copy in loads:
        copy.start()

    barrier = pltpu.get_barrier_semaphore()
    for d in range(1, n_dev):
        pl.semaphore_signal(barrier, inc=1, device_id={'cp': lax.rem(me + d, n_dev)}, device_id_type=pl.DeviceIdType.MESH)
    acc[...] = jnp.zeros_like(acc)
    dq[...] = jnp.zeros_like(dq)
    pl.semaphore_wait(barrier, n_dev - 1)

    def remote(src, dst, send, recv, device):
        return pltpu.make_async_remote_copy(src_ref=src, dst_ref=dst, send_sem=send, recv_sem=recv,
                                            device_id=device, device_id_type=pl.DeviceIdType.MESH)

    def kv_copies(slot, src_slot, h, sem_row, device):
        span = pl.ds(h * half, half)
        return [remote(kv.at[src_slot, i, span], kv.at[slot, i, span],
                       kv_send.at[sem_row, h, i], kv_recv.at[slot, h, i], device) for i in range(2)]

    def give_kv(to_chip, h):
        for copy in kv_copies(chip, own_slot + core, h, to_chip - 1, at(to_chip)):
            copy.start()

    def kv_sent(row):
        for h in range(2):
            for copy in kv_copies(0, 0, h, row, at(chip)):
                copy.wait_send()

    def kv_send_far():
        for h in range(2):
            give_kv(last, h)

    first_far = jnp.logical_or(jnp.logical_and(chip == 0, core == 0), jnp.logical_and(chip == last - 1, core == 1))
    loads[0].wait()
    loads[1].wait()

    @pl.when(first_far)
    def _():
        kv_send_far()

    @pl.when(chip == 0)
    def _():
        for h in range(2):
            give_kv(1, h)

        @pl.when(core == 0)
        def _():
            for h in range(2):
                give_kv(2, h)

    @pl.when(chip == 1)
    def _():
        for h in range(2):
            give_kv(2, h)

    def pair_copies(c):
        refs = (q.at[c], do.at[c], kv.at[own_slot + c, 0], kv.at[own_slot + c, 1], stats.at[c])
        return [remote(ref, ref, pair_send.at[i], pair_recv.at[i], partner) for i, ref in enumerate(refs)]

    def guest_copies(to_chip):
        n = n_guest[to_chip]
        src, dst = pl.ds(rows - n, n), pl.ds(0, n)
        pairs = ((q.at[core, :, src], guest_q.at[:, dst]), (do.at[core, :, src], guest_do.at[:, dst]),
                 (stats.at[core, :, src], guest_stats.at[:, dst]))
        return [remote(src, dst, guest_send.at[to_chip, i], guest_recv.at[i], at(to_chip))
                for i, (src, dst) in enumerate(pairs)]

    guests = [guest_copies(to_chip) for to_chip in range(2)]

    def guests_back(from_chip):
        span = pl.ds(0, n_guest[from_chip])
        return remote(guest_dq.at[:, span], back_dq.at[from_chip, :, span],
                      d_send.at[2], back_recv.at[from_chip], at(last))

    pair = pair_copies(core)
    for i in (2, 3):
        loads[i].wait()

        @pl.when(chip == last)
        def _():
            for copies in guests:
                copies[i - 2].start()

        pair[i - 2].start()
    pair[2].start()
    pair[3].start()
    loads[4].wait()
    loads[5].wait()
    for g in range(heads):
        stats[core, g:g + 1, :] = lse[g:g + 1, :] * LOG2E
        product = do[core, g].astype(jnp.float32) * fo[g].astype(jnp.float32)
        stats[core, heads + g:heads + g + 1, :] = jnp.sum(product.T, axis=0, keepdims=True)
    pair[4].start()

    @pl.when(chip == last)
    def _():
        for copies in guests:
            copies[2].start()

    def spread(row):
        return jnp.broadcast_to(row, (dim, row.shape[1])).T

    def prep(b):
        qt[b] = q[b].reshape(heads * rows, dim).T
        dot_t[b] = do[b].reshape(heads * rows, dim).T
        for g in range(heads):
            lseb[b, g] = spread(stats[b, g:g + 1, :])
            delb[b, g] = spread(stats[b, heads + g:heads + g + 1, :])

    def pair_grads(q_rows, do_rows, q_cols, do_cols, lse_rows, del_rows, kk, vv, size, masked):
        wide = lambda x: jnp.concatenate([x] * (kk.shape[0] // dim), axis=1)
        logits = dot(q_rows, kk, NT)
        prob = jnp.exp2(logits * scale2 - wide(lse_rows))
        if masked:
            row = lax.broadcasted_iota(jnp.int32, prob.shape, 0) & (size - 1)
            col = lax.broadcasted_iota(jnp.int32, prob.shape, 1)
            prob = jnp.where(col <= row, prob, 0.0)
        d_prob = dot(do_rows, vv, NT)
        score = (prob * (d_prob - wide(del_rows))).astype(jnp.bfloat16)
        prob = prob.astype(jnp.bfloat16)
        return dot(q_cols, score, NN), dot(do_cols, prob, NN), dot(score, kk, NN)

    def tile(blocks, first, size, slot, h, masked=False):
        start = pl.multiple_of(h * half, half)
        kk = kv[slot, 0, pl.ds(start, half), :]
        vv = kv[slot, 1, pl.ds(start, half), :]
        part = lambda ref: jnp.concatenate(
            [ref[b, :, first:first + size, :].reshape(heads * size, dim) for b in blocks], axis=0)
        part_t = lambda ref: jnp.concatenate(
            [ref[b, :, g * rows + first:g * rows + first + size] for b in blocks for g in range(heads)], axis=1)
        d_key, d_value, d_query = pair_grads(
            part(q), part(do), part_t(qt), part_t(dot_t), part(lseb), part(delb), kk, vv, size, masked)
        acc[slot, h, 0] += d_key
        acc[slot, h, 1] += d_value
        for i, b in enumerate(blocks):
            n = heads * size
            dq[b, :, first:first + size, :] += d_query[i * n:(i + 1) * n].reshape(heads, size, dim)

    def own_low():
        tile((core,), half, half, own_slot + core, 0)

    def partner_masked():
        tile((other,), half, half, own_slot + other, 1, masked=True)

    def square():
        tile((1,), 0, rows, own_slot, core)

    prep(core)
    tile((core,), 0, half, own_slot + core, 0, masked=True)

    @pl.when(core == 1)
    def _():
        own_low()

    for copy in pair_copies(other):
        copy.wait_recv()

    @pl.when(jnp.logical_and(chip == 0, core == 1))
    def _():
        kv_send_far()

    prep(other)

    @pl.when(core == 0)
    def _():
        partner_masked()

    def host(to_chip):
        for copy in guests[to_chip]:
            copy.wait_recv()
        size = n_guest[to_chip]
        n = heads * size
        flat = lambda ref: ref[:, :size, :].reshape(n, dim)
        guest_qt[:, :n] = flat(guest_q).T
        guest_dot[:, :n] = flat(guest_do).T
        for g in range(heads):
            guest_lse[g, :size] = spread(guest_stats[g:g + 1, :size])
            guest_del[g, :size] = spread(guest_stats[heads + g:heads + g + 1, :size])
        guest_dq[:, :size] = jnp.zeros((heads, size, dim), jnp.float32)

        @pl.loop(0, 2)
        def _(b):
            d_key, d_value, d_query = pair_grads(
                flat(guest_q), flat(guest_do), guest_qt[:, :n], guest_dot[:, :n], flat(guest_lse), flat(guest_del),
                kv[own_slot + b, 0], kv[own_slot + b, 1], size, False)
            for h in range(2):
                acc[own_slot + b, h, 0] += d_key[:, h * half:(h + 1) * half]
                acc[own_slot + b, h, 1] += d_value[:, h * half:(h + 1) * half]
            guest_dq[:, :size] += d_query.reshape(heads, size, dim)

        guests_back(to_chip).start()

    def arrived(from_slot, part):
        for copy in kv_copies(from_slot, own_slot + core, part, 0, at(chip)):
            copy.wait_recv()

    def pass_on(from_slot, part, to_chip):
        for copy in kv_copies(from_slot, from_slot, part, from_slot, at(to_chip)):
            copy.start()

    relays_kv = jnp.logical_and(chip == 1, core == 1)

    @pl.when(relays_kv)
    def _():
        for part in range(2):
            arrived(0, part)
            pass_on(0, part, 2)

    for to_chip in range(2):
        @pl.when(chip == to_chip)
        def _():
            host(to_chip)

    def g_copy(slot, h, buf, to_chip):
        return remote(acc.at[slot, h], rbuf.at[buf, h], g_send.at[slot, h], g_recv.at[buf, h], at(to_chip))

    def g_wait(buf, h):
        g_copy(0, h, buf, chip).wait_recv()

    def add_relayed(slot, h):
        g_wait(R, h)
        acc[slot, h] += rbuf[R, h]

    def send_partial(slot, h):
        @pl.when(jnp.logical_and(chip == 1, core == 1))
        def _():
            g_copy(slot, h, A, 0).start()

        @pl.when(chip == 2)
        def _():
            @pl.when(jnp.logical_and(slot == 1, core == 1))
            def _():
                g_copy(slot, h, A, 1).start()

            @pl.when(jnp.logical_and(slot == 0, core == 0))
            def _():
                g_copy(slot, h, R, 1).start()

            @pl.when(jnp.logical_and(slot == 0, core == 1))
            def _():
                g_copy(slot, h, R, 3).start()

        @pl.when(chip == 3)
        def _():
            @pl.when(jnp.logical_and(slot == 0, core == 0))
            def _():
                g_copy(slot, h, B, 0).start()

            @pl.when(jnp.logical_and(slot == 0, core == 1))
            def _():
                add_relayed(slot, h)
                g_copy(slot, h, B, 0).start()

            @pl.when(jnp.logical_and(slot == 1, core == 0))
            def _():
                g_copy(slot, h, R, 2).start()

            @pl.when(jnp.logical_and(slot == 1, core == 1))
            def _():
                g_copy(slot, h, R, 0).start()

            @pl.when(slot == 2)
            def _():
                g_copy(slot, h, A, 2).start()

    @pl.loop(0, 2 * chip)
    def _(u):
        near_first = jnp.where(jnp.logical_and(chip == last, core == 0), u // 2, chip - 1 - u // 2)
        far_inside = chip == last - 1
        inside = jnp.logical_and(far_inside, core == 0)
        slot = jnp.where(inside, jnp.where(jnp.logical_or(u == 0, u == 3), 1, 0), near_first)
        h = jnp.where(inside, u // 2, u % 2)

        awaited_before = jnp.logical_or(relays_kv, jnp.logical_and(far_inside, jnp.logical_and(slot == 1, h == 1)))

        @pl.when(jnp.logical_and(far_inside, u == 1))
        def _():
            arrived(1, 1)
            pass_on(1, 1, last)

        @pl.when(jnp.logical_not(awaited_before))
        def _():
            arrived(slot, h)

        @pl.when(jnp.logical_and(far_inside, u == 0))
        def _():
            pass_on(1, 0, last)

            @pl.when(core == 0)
            def _():
                kv_send_far()

        without_guests = jnp.logical_and(chip == last, slot < 2)
        for to_chip in range(2):
            @pl.when(jnp.logical_and(chip == last, slot == to_chip))
            def _():
                @pl.loop(0, 2)
                def _(b):
                    tile((b,), 0, rows - n_guest[to_chip], slot, h)

        @pl.when(jnp.logical_not(without_guests))
        def _():
            @pl.loop(0, 2)
            def _(b):
                tile((b,), 0, rows, slot, h)

        send_partial(slot, h)

    relay_add = jnp.logical_and(jnp.logical_or(chip == 1, chip == 2), core == 0)
    relay_pass = jnp.logical_and(chip == 0, core == 1)

    def pass_copy(h):
        return remote(rbuf.at[R, h], rbuf.at[B, h], f_send.at[h], g_recv.at[B, h], at(1))

    def relay(h):
        @pl.when(relay_add)
        def _():
            add_relayed(chip - 1, h)
            g_copy(chip - 1, h, A, chip - 1).start()

    swaps = [remote(acc.at[own_slot + other, h], rhalf.at[h], d_send.at[3 * h], d_recv.at[3 * h], partner)
             for h in range(2)]
    give_dq = remote(dq.at[other], rdq, d_send.at[1], d_recv.at[1], partner)

    relay(0)

    @pl.when(core == 0)
    def _():
        swaps[1].start()
        square()

    @pl.when(core == 1)
    def _():
        partner_masked()

    give_dq.start()
    relay(1)

    @pl.when(core == 0)
    def _():
        own_low()

    @pl.when(core == 1)
    def _():
        square()
        swaps[1].start()

    @pl.when(chip < 2)
    def _():
        swaps[0].start()

    give_dq.wait_recv()
    for g in range(heads):
        out[g] = ((dq[core, g] + rdq[g]) * scale).astype(out.dtype)

    @pl.when(chip == last)
    def _():
        for from_chip in range(2):
            guests_back(from_chip).wait_recv()
        for g in range(heads):
            for n in (n_guest[0], n_guest[1]):
                first = rows - n
                total = dq[core, g, first:, :] + rdq[g, first:, :] + back_dq[0, g, n_guest[0] - n:, :]
                if n == n_guest[1]:
                    total = total + back_dq[1, g, :n, :]
                out[g, first:, :] = (total * scale).astype(out.dtype)

    @pl.when(relay_pass)
    def _():
        for h in range(2):
            g_wait(R, h)
            pass_copy(h).start()

    @pl.when(chip < 2)
    def _():
        swaps[0].wait_recv()
        acc[own_slot + core, 0] += rhalf[0]

    swaps[1].wait_recv()
    acc[own_slot + core, 1] += rhalf[1]
    from_b = jnp.logical_or(chip == 0, jnp.logical_and(chip == 1, core == 1))
    for h in range(2):
        @pl.when(chip < last)
        def _():
            g_wait(A, h)
            acc[own_slot + core, h] += rbuf[A, h]

        @pl.when(from_b)
        def _():
            g_wait(B, h)
            acc[own_slot + core, h] += rbuf[B, h]

        out[heads, h * half:(h + 1) * half, :] = (acc[own_slot + core, h, 0].T * scale).astype(out.dtype)
        out[heads + 1, h * half:(h + 1) * half, :] = acc[own_slot + core, h, 1].T.astype(out.dtype)

    for copy in pair:
        copy.wait_send()
    give_dq.wait_send()
    swaps[1].wait_send()

    @pl.when(chip < 2)
    def _():
        swaps[0].wait_send()

    for from_chip in range(2):
        @pl.when(chip == from_chip)
        def _():
            guests_back(from_chip).wait_send()

    @pl.when(chip == last)
    def _():
        for copies in guests:
            for copy in copies:
                copy.wait_send()

    @pl.when(jnp.logical_or(chip == 0, chip == last - 1))
    def _():
        kv_sent(last - 1)

    @pl.when(jnp.logical_and(chip < last, me != 1))
    def _():
        kv_sent(1)

    @pl.when(jnp.logical_or(chip == 0, me == 3))
    def _():
        kv_sent(0)

    @pl.loop(0, chip)
    def _(slot):
        for h in range(2):
            g_copy(slot, h, A, chip).wait_send()

    @pl.when(relay_pass)
    def _():
        for h in range(2):
            pass_copy(h).wait_send()


def unpack_kernel(packed, gq, gk, gv, out_sem):
    heads = gq.shape[0]
    outs = [gq, gk, gv]
    parts = [packed.at[0:heads], packed.at[heads], packed.at[heads + 1]]
    writes = [pltpu.make_async_copy(part, dst, out_sem.at[i]) for i, (part, dst) in enumerate(zip(parts, outs))]
    for copy in writes:
        copy.start()
    for copy in writes:
        copy.wait()


def solution(mesh):
    n_dev = mesh.shape['cp']
    row_spec = P(('dp', 'cp'))

    def local_fn(q_tok, k_tok, v_tok, fwd_out, d_out, lse_row):
        rows, heads, dim = q_tok.shape
        half = rows // 2
        n_guest = (3 * rows // 8, rows // 4)
        most = max(n_guest)
        n_slot = n_dev // 2 + 2
        bf16, f32 = jnp.bfloat16, jnp.float32
        any_spec = pl.BlockSpec(memory_space=pl.ANY)
        dma = pltpu.SemaphoreType.DMA
        vmem = pltpu.VMEM
        packed = pl.pallas_call(
            functools.partial(kernel, n_dev, n_guest),
            out_shape=vmem((heads + 2, rows, dim), bf16),
            in_specs=[any_spec] * 6,
            out_specs=pl.BlockSpec(memory_space=vmem),
            scratch_shapes=[
                vmem((2, heads, rows, dim), bf16), vmem((2, heads, rows, dim), bf16),
                vmem((heads, rows, dim), bf16), vmem((heads, rows), f32), vmem((2, 8, rows), f32),
                vmem((2, dim, heads * rows), bf16), vmem((2, dim, heads * rows), bf16),
                vmem((2, heads, rows, dim), f32), vmem((2, heads, rows, dim), f32),
                vmem((n_slot, 2, rows, dim), bf16),
                vmem((n_slot, 2, 2, dim, half), f32),
                vmem((2, heads, rows, dim), f32),
                vmem((3, 2, 2, dim, half), f32), vmem((2, 2, dim, half), f32),
                vmem((heads, rows, dim), f32),
                vmem((heads, most, dim), bf16), vmem((heads, most, dim), bf16), vmem((8, most), f32),
                vmem((dim, heads * most), bf16), vmem((dim, heads * most), bf16),
                vmem((heads, most, dim), f32), vmem((heads, most, dim), f32),
                vmem((heads, most, dim), f32), vmem((2, heads, most, dim), f32),
                dma((6,)), dma((5,)), dma((5,)),
                dma((3, 2, 2)), dma((n_slot, 2, 2)),
                dma((n_slot, 2)), dma((3, 2)), dma((2,)), dma((4,)), dma((4,)),
                dma((2, 3)), dma((3,)), dma((2,)),
            ],
            compiler_params=pltpu.CompilerParams(
                collective_id=0, has_side_effects=True, vmem_limit_bytes=56 * 2 ** 20),
            name='attn_bwd',
        )(q_tok.transpose(1, 0, 2), d_out.transpose(1, 0, 2), fwd_out.transpose(1, 0, 2), lse_row.T, k_tok, v_tok)
        gq, gk, gv = pl.pallas_call(
            unpack_kernel,
            out_shape=[
                jax.ShapeDtypeStruct((heads, rows, dim), bf16),
                jax.ShapeDtypeStruct((rows, dim), bf16),
                jax.ShapeDtypeStruct((rows, dim), bf16),
            ],
            in_specs=[pl.BlockSpec(memory_space=vmem)],
            out_specs=[any_spec] * 3,
            scratch_shapes=[dma((3,))],
            name='unpack',
        )(pltpu.with_memory_space_constraint(packed, pltpu.VMEM))
        return gq.transpose(1, 0, 2), gk, gv

    return jax.shard_map(local_fn, mesh=mesh, in_specs=(row_spec,) * 6, out_specs=(row_spec,) * 3, check_vma=False)
```
